256 devices in a mesh: rows: 32 (over x, y, core), grp: 8 (over z).
Axes of the slice: x: 4, y: 4, z: 8, core: 2. Of those that a mesh axis runs over, the one named last changes fastest.
Arguments:
- factor: float32 [65536, 1024], P(('rows', 'grp')), as said below
- start_block: float32 [1024, 256], replicated, may hold values from -6 to 6
Outputs:
- compressed: float32 [65536, 256], P(('rows', 'grp'))
- tail_share: float32 [], replicated
The draws below stay inside these ranges and needn't reach their ends.
Inputs may be any that keep to these rules, and one draw needn't show every extreme that they name: Every entry is finite; the factor has full column rank.
All inputs are finite; a program needn't handle non-finite values.
Results may differ from the reference program's by a relative error of at most 0.0007.
Values sent between devices are 32-bit elements; how exact they have to be, the bound alone decides.
A program may use at most 64 MiB of HBM per device.

```python
import math
import jax
import jax.numpy as jnp
from jax import lax

K = 1024
RANK = 256
ITERS = 1
ROWS_ALL = 65536


def draw_factor(key, part):
    keys = jax.random.split(key, 3)
    position = jnp.arange(ROWS_ALL, dtype=jnp.float32) / ROWS_ALL
    row_scale = jnp.exp(jax.random.uniform(keys[0], (ROWS_ALL,), jnp.float32) * math.log(10.0)) * (1.0 + 2.0 * position)
    col_scale = jnp.exp(jax.random.uniform(keys[1], (K,), jnp.float32) * math.log(10.0))
    noise = jax.random.normal(keys[2], (ROWS_ALL, K), jnp.float32)
    return (0.1 * row_scale[:, None] * col_scale[None, :] * noise).astype(jnp.float32)


def normal_values(own_key, shape, width, reach, kind=jnp.bfloat16):
    array = jax.random.normal(own_key, shape, jnp.float32) * width
    return jnp.minimum(jnp.maximum(array, -reach), reach).astype(kind)


def setup_inputs(seed: int = 0) -> dict:
    streams_of = jax.random.split(jax.random.key(seed), 3)
    return {
        "factor": draw_factor(jax.random.fold_in(streams_of[2], 71), 0),
        "start_block": normal_values(streams_of[1], (K, RANK), 1.0, 6.0, jnp.float32),
    }


def orthonormal(columns):
    product = jnp.dot(columns.T, columns, precision=lax.Precision.HIGHEST)
    lower_factor = jnp.linalg.cholesky(product)
    return jax.scipy.linalg.solve_triangular(lower_factor, columns.T, lower=True).T

def reference(factor, start_block):
    gram_total = jnp.dot(factor.T, factor, precision=lax.Precision.HIGHEST)
    basis_now = orthonormal(start_block)
    for iteration in range(ITERS):
        basis_now = orthonormal(jnp.dot(gram_total, basis_now, precision=lax.Precision.HIGHEST))
    compressed = jnp.dot(factor, basis_now, precision=lax.Precision.HIGHEST)
    kept_energy = jnp.sum(basis_now * jnp.dot(gram_total, basis_now, precision=lax.Precision.HIGHEST))
    total_energy = jnp.trace(gram_total)
    tail_share = (1.0 - kept_energy / total_energy).astype(jnp.float32)
    return (compressed, tail_share)
```

```python
import jax
import jax.numpy as jnp
from jax import lax
from jax.sharding import PartitionSpec as P

AXES = ("rows", "grp")
HI = lax.Precision.HIGHEST


def dot(a, b):
    return jnp.dot(a, b, precision=HI)


def local(factor, start_block):
    image = dot(factor.T, dot(factor, start_block))
    image = lax.psum(image, AXES)
    first = jnp.linalg.cholesky(dot(start_block.T, start_block))
    eye = jnp.eye(first.shape[0], dtype=jnp.float32)
    first_inv = jax.scipy.linalg.solve_triangular(first, eye, lower=True)
    image = dot(image, first_inv.T)
    second = jnp.linalg.cholesky(dot(image.T, image))
    projected = dot(factor, image)
    compressed = jax.scipy.linalg.solve_triangular(second, projected.T, lower=True).T
    energies = lax.psum(jnp.stack([jnp.sum(compressed * compressed), jnp.sum(factor * factor)]), AXES)
    tail_share = (1.0 - energies[0] / energies[1]).astype(jnp.float32)
    return (compressed, tail_share)


def solution(mesh):
    in_specs = (P(AXES, None), P())
    out_specs = (P(AXES, None), P())
    return jax.shard_map(local, mesh=mesh, in_specs=in_specs, out_specs=out_specs, check_vma=False)
```

```python
import functools
import math

import jax
import jax.numpy as jnp
from jax import lax
from jax.experimental import pallas as pl
from jax.experimental.pallas import tpu as pltpu
from jax.sharding import PartitionSpec as P

AXES = ("rows", "grp")
HI = lax.Precision.HIGHEST
B = 16
F32 = jnp.float32


def contract(a, b, da, db):
    return lax.dot_general(a, b, (((da,), (db,)), ((), ())), precision=HI, preferred_element_type=F32)


def split3(x):
    a = x.astype(jnp.bfloat16).astype(F32)
    rest = x - a
    b = rest.astype(jnp.bfloat16).astype(F32)
    return a, b, (rest - b).astype(jnp.bfloat16).astype(F32)


def factor_step(m_ref, k):
    n = m_ref.shape[1]
    per = 128 // B
    row0 = pl.multiple_of(k * B, B)
    half = pl.multiple_of((k // per) * 128, 128)
    lane0 = (k % per) * B
    rows8 = lax.broadcasted_iota(jnp.int32, (8, 128), 0)
    diag = [m_ref[pl.ds(row0 + 8 * g, 8), pl.ds(half, 128)] for g in range(2)]
    column = {}
    for c in range(B):
        idx = jnp.full((8, 128), lane0 + c, jnp.int32)
        for g in range(2):
            if 8 * g + 8 > c:
                column[c, g] = jnp.take_along_axis(diag[g], idx, axis=1)
    lanes = lax.broadcasted_iota(jnp.int32, (8, n), 1) - k * B
    in_block = (lanes >= 0) & (lanes < B)
    wide = []
    for g in range(2):
        unit = jnp.where(lanes == 8 * g + lax.broadcasted_iota(jnp.int32, (8, n), 0), 1.0, 0.0)
        wide.append(jnp.where(in_block, unit, m_ref[pl.ds(row0 + 8 * g, 8), :]))
    pivots = [jnp.ones((8, 128), F32) for _ in range(2)]
    for c in range(B):
        gc, rc = divmod(c, 8)
        pivot = jnp.broadcast_to(column[c, gc][rc : rc + 1, :], (8, 128))
        pivots[gc] = jnp.where(rows8 == rc, pivot, pivots[gc])
        scale = 1.0 / pivot
        mult = {g: column[c, g] * scale for g in range(gc, 2)}
        mult[gc] = jnp.where(rows8 > rc, mult[gc], 0.0)
        pivot_row = jnp.broadcast_to(wide[gc][rc : rc + 1, :], (8, n))
        for d in range(c + 1, B):
            gd, rd = divmod(d, 8)
            entry = jnp.broadcast_to(column[c, gd][rd : rd + 1, :], (8, 128))
            for g in range(gd, 2):
                column[d, g] = column[d, g] - mult[g] * entry
        for g in range(gc, 2):
            wide[g] = wide[g] - jnp.tile(mult[g], (1, n // 128)) * pivot_row
    final = []
    for g in range(2):
        s = lax.rsqrt(pivots[g])
        s = s * (1.5 - 0.5 * pivots[g] * s * s)
        final.append(wide[g] * jnp.tile(s, (1, n // 128)))
    u = jnp.concatenate(final, axis=0)
    a, b, c = split3(u)
    right = jnp.concatenate([a, b, a, c, b, a], axis=0).astype(jnp.bfloat16)
    later = lax.broadcasted_iota(jnp.int32, (B, n), 1) >= (k + 1) * B
    a, b, c = (jnp.where(later, t, 0.0) for t in (a, b, c))
    left = jnp.concatenate([a, a, b, a, b, c], axis=0).T.astype(jnp.bfloat16)
    update = jnp.dot(left, right, preferred_element_type=F32)
    cols = lax.broadcasted_iota(jnp.int32, (n, n), 1) - k * B
    m_ref[...] = jnp.where((cols >= 0) & (cols < B), 0.0, m_ref[...]) - update
    m_ref[pl.ds(row0, B), :] = u


def factor_steps(m_ref, lo, hi):
    def body(k, carry):
        factor_step(m_ref, k)
        return carry

    lax.fori_loop(lo, hi, body, 0)


def kernel(
    sizes,
    z_ref,
    s_ref,
    c_ref,
    tail_ref,
    w_ref,
    x_ref,
    pair_ref,
    plane_ref,
    slab_ref,
    line_ref,
    full_ref,
    m1_ref,
    m2_ref,
    e_ref,
    ep_ref,
    eq_ref,
    *sems,
):
    nx, ny, nz = sizes
    (pair_s, pair_r, plane_s, plane_r, line_s, line_r, zg_s, zg_r, pg_s, pg_r, fw_s, fw_r, ep_s, ep_r, eq_s, eq_r) = sems
    nq = nx * ny
    rank, depth = s_ref.shape[1], s_ref.shape[0]
    half = rank // 2
    rows, cols = half // nq, depth // nz
    me = lax.axis_index("rows")
    mz = lax.axis_index("grp")
    mc = me % 2
    mq = me // 2
    mx, my = mq // ny, mq % ny

    def at(q, c, z):
        return {"rows": q * 2 + c, "grp": z}

    def plane_peer(dx, dy):
        return ((mx + dx) % nx) * ny + (my + dy) % ny

    far = lambda d, n: min(d, n - d)
    plane = [(dx, dy) for dx in range(nx) for dy in range(ny) if dx or dy]
    plane.sort(key=lambda d: (-far(d[0], nx) - far(d[1], ny), d))
    line = sorted(range(1, nz), key=lambda d: (-far(d, nz), d))
    other = 1 - mc

    barrier = pltpu.get_barrier_semaphore()
    greet = [at(mq, other, mz)]
    greet += [at(plane_peer(dx, dy), mc, mz) for dx, dy in plane]
    greet += [at(mq, mc, (mz + dz) % nz) for dz in line]
    greet += [at(mq, other, (mz + dz) % nz) for dz in line]
    for device in greet:
        pl.semaphore_signal(barrier, inc=1, device_id=device, device_id_type=pl.DeviceIdType.MESH)

    def remote(src, dst, send, recv, device):
        return pltpu.make_async_remote_copy(
            src_ref=src, dst_ref=dst, send_sem=send, recv_sem=recv, device_id=device, device_id_type=pl.DeviceIdType.MESH
        )

    def half_rows(c):
        return pl.ds(pl.multiple_of(c * half, half), half)

    def slab_rows(c, q):
        return pl.ds(pl.multiple_of(c * half + q * rows, rows), rows)

    def slab_cols(z):
        return pl.ds(pl.multiple_of(z * cols, cols), cols)

    w_ref[...] = contract(z_ref[...], s_ref[...], 1, 0)
    x_ref[half_rows(other), :] = contract(w_ref[:, half_rows(other)], z_ref[...], 0, 0)
    pl.semaphore_wait(barrier, len(greet))
    pair = remote(x_ref.at[half_rows(other), :], pair_ref, pair_s, pair_r, at(mq, other, mz))
    pair.start()
    x_ref[half_rows(mc), :] = contract(w_ref[:, half_rows(mc)], z_ref[...], 0, 0)
    pair.wait()
    x_ref[half_rows(mc), :] = x_ref[half_rows(mc), :] + pair_ref[...]

    copies = []
    for j, (dx, dy) in enumerate(plane):
        q = plane_peer(dx, dy)
        copies.append(remote(x_ref.at[slab_rows(mc, q), :], plane_ref.at[j], plane_s.at[j], plane_r.at[j], at(q, mc, mz)))
        copies[-1].start()
    m1_ref[...] = contract(s_ref[...], s_ref[...], 0, 0)
    steps = rank // B
    cut1, cut2, cut3 = steps * 7 // 16, steps * 11 // 16, steps
    factor_steps(m1_ref, 0, cut1)
    total = x_ref[slab_rows(mc, mq), :]
    for j, copy in enumerate(copies):
        copy.wait_recv()
        total = total + plane_ref[j]
    slab_ref[...] = total
    lines = []
    for j, dz in enumerate(line):
        z = (mz + dz) % nz
        lines.append(remote(slab_ref.at[:, slab_cols(z)], line_ref.at[j], line_s.at[j], line_r.at[j], at(mq, mc, z)))
        lines[-1].start()
    factor_steps(m1_ref, cut1, cut2)
    total = slab_ref[:, slab_cols(mz)]
    for j, copy in enumerate(lines):
        copy.wait_recv()
        total = total + line_ref[j]
    full_ref[slab_rows(mc, mq), slab_cols(mz)] = total

    tile = full_ref.at[slab_rows(mc, mq), slab_cols(mz)]
    tiles = []
    for j, dz in enumerate(line):
        tiles.append(remote(tile, tile, zg_s.at[j], zg_r.at[j], at(mq, mc, (mz + dz) % nz)))
        tiles[-1].start()
    factor_steps(m1_ref, cut2, cut3)
    for copy in tiles:
        copy.wait_recv()
    slab = full_ref.at[slab_rows(mc, mq), :]
    slabs = []
    for j, (dx, dy) in enumerate(plane):
        slabs.append(remote(slab, slab, pg_s.at[j], pg_r.at[j], at(plane_peer(dx, dy), mc, mz)))
        slabs[-1].start()
    forwards = [remote(slab, slab, fw_s.at[nq - 1], fw_r.at[nq - 1], at(mq, other, mz))]
    forwards[0].start()
    energy_all = jnp.sum(z_ref[...] * z_ref[...])
    for j in reversed(range(len(plane))):
        dx, dy = plane[j]
        slabs[j].wait_recv()
        block = full_ref.at[slab_rows(mc, plane_peer(-dx, -dy)), :]
        forwards.append(remote(block, block, fw_s.at[j], fw_r.at[j], at(mq, other, mz)))
        forwards[-1].start()
    for copy in forwards:
        copy.wait_recv()
    for copy in copies:
        copy.wait_send()

    x_ref[...] = contract(m1_ref[...], full_ref[...], 1, 0)
    m2_ref[...] = contract(x_ref[...], x_ref[...], 1, 1)
    w_ref[...] = contract(z_ref[...], x_ref[...], 1, 1)
    factor_steps(m2_ref, 0, steps)
    compressed = contract(w_ref[...], m2_ref[...], 1, 1)
    c_ref[...] = compressed
    energy_kept = jnp.sum(compressed * compressed)

    lane = lax.broadcasted_iota(jnp.int32, (1, 128), 1)
    e_ref[...] = jnp.where(lane == 0, energy_kept, jnp.where(lane == 1, energy_all, 0.0))
    ep_ref[mq] = e_ref[...]
    first = []
    for j, (dx, dy) in enumerate(plane):
        first.append(remote(e_ref, ep_ref.at[mq], ep_s.at[j], ep_r.at[j], at(plane_peer(dx, dy), mc, mz)))
        first[-1].start()
    for copy in first:
        copy.wait()
    e_ref[...] = functools.reduce(jnp.add, [ep_ref[q] for q in range(nq)])
    spot = mz * 2 + mc
    eq_ref[spot] = e_ref[...]
    second = []
    for j, (dz, dc) in enumerate([(dz, dc) for dc in range(2) for dz in [*line, 0] if dz or dc]):
        second.append(
            remote(e_ref, eq_ref.at[spot], eq_s.at[j], eq_r.at[j], at(mq, (mc + dc) % 2, (mz + dz) % nz))
        )
        second[-1].start()
    for copy in second:
        copy.wait()
    sums = functools.reduce(jnp.add, [eq_ref[i] for i in range(2 * nz)])
    tail_ref[...] = 1.0 - sums[:, 0:1] / sums[:, 1:2]
    for copy in [*lines, *tiles, *slabs, *forwards]:
        copy.wait_send()


def local(sizes, factor, start_block):
    nx, ny, nz = sizes
    nq = nx * ny
    depth, rank = start_block.shape
    half = rank // 2
    rows, cols = half // nq, depth // nz
    vmem = pl.BlockSpec(memory_space=pltpu.VMEM)
    dma = pltpu.SemaphoreType.DMA
    compressed, tail = pl.pallas_call(
        functools.partial(kernel, sizes),
        out_shape=(
            jax.ShapeDtypeStruct((factor.shape[0], rank), F32),
            jax.ShapeDtypeStruct((1, 1), F32),
        ),
        in_specs=[vmem, vmem],
        out_specs=(vmem, vmem),
        scratch_shapes=[
            pltpu.VMEM((factor.shape[0], rank), F32),
            pltpu.VMEM((rank, depth), F32),
            pltpu.VMEM((half, depth), F32),
            pltpu.VMEM((nq - 1, rows, depth), F32),
            pltpu.VMEM((rows, depth), F32),
            pltpu.VMEM((nz - 1, rows, cols), F32),
            pltpu.VMEM((rank, depth), F32),
            pltpu.VMEM((rank, rank), F32),
            pltpu.VMEM((rank, rank), F32),
            pltpu.VMEM((1, 128), F32),
            pltpu.VMEM((nq, 1, 128), F32),
            pltpu.VMEM((2 * nz, 1, 128), F32),
            dma,
            dma,
            dma((nq - 1,)),
            dma((nq - 1,)),
            dma((nz - 1,)),
            dma((nz - 1,)),
            dma((nz - 1,)),
            dma((nz - 1,)),
            dma((nq - 1,)),
            dma((nq - 1,)),
            dma((nq,)),
            dma((nq,)),
            dma((nq - 1,)),
            dma((nq - 1,)),
            dma((2 * nz - 1,)),
            dma((2 * nz - 1,)),
        ],
        compiler_params=pltpu.CompilerParams(
            collective_id=0, has_side_effects=True, vmem_limit_bytes=40 * 2**20
        ),
    )(factor, start_block)
    return compressed, tail[0, 0]


def solution(mesh):
    side = math.isqrt(mesh.shape["rows"] // 2)
    sizes = (side, side, mesh.shape["grp"])
    return jax.shard_map(
        functools.partial(local, sizes),
        mesh=mesh,
        in_specs=(P(AXES, None), P()),
        out_specs=(P(AXES, None), P()),
        check_vma=False,
    )
```

```python
import functools
import math

import jax
import jax.numpy as jnp
from jax import lax
from jax.experimental import pallas as pl
from jax.experimental.pallas import tpu as pltpu
from jax.sharding import PartitionSpec as P

AXES = ("rows", "grp")
HI = lax.Precision.HIGHEST
B = 16
F32 = jnp.float32
PARTS = 4
CUT1, CUT2 = 9, 12


def contract(a, b, da, db):
    return lax.dot_general(a, b, (((da,), (db,)), ((), ())), precision=HI, preferred_element_type=F32)


def split3(x):
    a = x.astype(jnp.bfloat16).astype(F32)
    rest = x - a
    b = rest.astype(jnp.bfloat16).astype(F32)
    return a, b, (rest - b).astype(jnp.bfloat16).astype(F32)


def factor_step(m_ref, k):
    n = m_ref.shape[1]
    per = 128 // B
    row0 = pl.multiple_of(k * B, B)
    half = pl.multiple_of((k // per) * 128, 128)
    lane0 = (k % per) * B
    rows8 = lax.broadcasted_iota(jnp.int32, (8, 128), 0)
    diag = [m_ref[pl.ds(row0 + 8 * g, 8), pl.ds(half, 128)] for g in range(2)]
    column = {}
    for c in range(B):
        idx = jnp.full((8, 128), lane0 + c, jnp.int32)
        for g in range(2):
            if 8 * g + 8 > c:
                column[c, g] = jnp.take_along_axis(diag[g], idx, axis=1)
    lanes = lax.broadcasted_iota(jnp.int32, (8, n), 1) - k * B
    in_block = (lanes >= 0) & (lanes < B)
    wide = []
    for g in range(2):
        unit = jnp.where(lanes == 8 * g + lax.broadcasted_iota(jnp.int32, (8, n), 0), 1.0, 0.0)
        wide.append(jnp.where(in_block, unit, m_ref[pl.ds(row0 + 8 * g, 8), :]))
    pivots = [jnp.ones((8, 128), F32) for _ in range(2)]
    for c in range(B):
        gc, rc = divmod(c, 8)
        pivot = jnp.broadcast_to(column[c, gc][rc : rc + 1, :], (8, 128))
        pivots[gc] = jnp.where(rows8 == rc, pivot, pivots[gc])
        scale = 1.0 / pivot
        mult = {g: column[c, g] * scale for g in range(gc, 2)}
        mult[gc] = jnp.where(rows8 > rc, mult[gc], 0.0)
        pivot_row = jnp.broadcast_to(wide[gc][rc : rc + 1, :], (8, n))
        for d in range(c + 1, B):
            gd, rd = divmod(d, 8)
            entry = jnp.broadcast_to(column[c, gd][rd : rd + 1, :], (8, 128))
            for g in range(gd, 2):
                column[d, g] = column[d, g] - mult[g] * entry
        for g in range(gc, 2):
            wide[g] = wide[g] - jnp.tile(mult[g], (1, n // 128)) * pivot_row
    final = []
    for g in range(2):
        s = lax.rsqrt(pivots[g])
        s = s * (1.5 - 0.5 * pivots[g] * s * s)
        final.append(wide[g] * jnp.tile(s, (1, n // 128)))
    u = jnp.concatenate(final, axis=0)
    a, b, c = split3(u)
    right = jnp.concatenate([a, b, a, c, b, a], axis=0).astype(jnp.bfloat16)
    later = lax.broadcasted_iota(jnp.int32, (B, n), 1) >= (k + 1) * B
    a, b, c = (jnp.where(later, t, 0.0) for t in (a, b, c))
    left = jnp.concatenate([a, a, b, a, b, c], axis=0).T.astype(jnp.bfloat16)
    update = jnp.dot(left, right, preferred_element_type=F32)
    cols = lax.broadcasted_iota(jnp.int32, (n, n), 1) - k * B
    m_ref[...] = jnp.where((cols >= 0) & (cols < B), 0.0, m_ref[...]) - update
    m_ref[pl.ds(row0, B), :] = u


def factor_steps(m_ref, lo, hi):
    def body(k, carry):
        factor_step(m_ref, k)
        return carry

    lax.fori_loop(lo, hi, body, 0)


def kernel(
    sizes,
    z_hbm,
    s_hbm,
    c_ref,
    tail_ref,
    z_ref,
    s_ref,
    w_ref,
    x_ref,
    pair_ref,
    plane_ref,
    line_ref,
    full_ref,
    part_ref,
    m1_ref,
    m2_ref,
    e_ref,
    ep_ref,
    eq_ref,
    *sems,
):
    nx, ny, nz = sizes
    (z_in, s_in, pair_s, pair_r, plane_s, plane_r, line_s, line_r, back_s, back_r, fw_s, fw_r, ep_s, ep_r, eq_s, eq_r) = sems
    nq = nx * ny
    rank, depth = s_ref.shape[1], s_ref.shape[0]
    half = rank // 2
    rows, cols = half // nq, depth // PARTS
    me = lax.axis_index("rows")
    mz = lax.axis_index("grp")
    mc = me % 2
    mq = me // 2
    mx, my = mq // ny, mq % ny

    def at(q, c, z):
        return {"rows": q * 2 + c, "grp": z}

    def plane_peer(dx, dy):
        return ((mx + dx) % nx) * ny + (my + dy) % ny

    far = lambda d, n: min(d, n - d)
    plane = [(dx, dy) for dx in range(nx) for dy in range(ny) if dx or dy]
    plane.sort(key=lambda d: (-far(d[0], nx) - far(d[1], ny), d))
    line = sorted(range(1, nz), key=lambda d: (-far(d, nz), d))
    other = 1 - mc

    def part(i):
        return pl.ds(i * cols, cols)

    loads = []
    for i in range(PARTS):
        loads.append(pltpu.make_async_copy(z_hbm.at[:, part(i)], z_ref.at[:, part(i)], z_in.at[i]))
        loads.append(pltpu.make_async_copy(s_hbm.at[part(i), :], s_ref.at[part(i), :], s_in.at[i]))
    for copy in loads:
        copy.start()

    barrier = pltpu.get_barrier_semaphore()
    greet = [at(mq, other, mz)]
    greet += [at(plane_peer(dx, dy), mc, mz) for dx, dy in plane]
    greet += [at(mq, mc, (mz + dz) % nz) for dz in line]
    greet += [at(mq, other, (mz + dz) % nz) for dz in line]
    for device in greet:
        pl.semaphore_signal(barrier, inc=1, device_id=device, device_id_type=pl.DeviceIdType.MESH)

    def remote(src, dst, send, recv, device):
        return pltpu.make_async_remote_copy(
            src_ref=src, dst_ref=dst, send_sem=send, recv_sem=recv, device_id=device, device_id_type=pl.DeviceIdType.MESH
        )

    def half_rows(c):
        return pl.ds(pl.multiple_of(c * half, half), half)

    def slab_rows(c, q):
        return pl.ds(pl.multiple_of(c * half + q * rows, rows), rows)

    for i in range(PARTS):
        loads[2 * i].wait()
        loads[2 * i + 1].wait()
        term = contract(z_ref[:, part(i)], s_ref[part(i), :], 1, 0)
        w_ref[...] = term if i == 0 else w_ref[...] + term
    x_ref[half_rows(other), :] = contract(w_ref[:, half_rows(other)], z_ref[...], 0, 0)
    pl.semaphore_wait(barrier, len(greet))
    pair = remote(x_ref.at[half_rows(other), :], pair_ref, pair_s, pair_r, at(mq, other, mz))
    pair.start()
    x_ref[half_rows(mc), :] = contract(w_ref[:, half_rows(mc)], z_ref[...], 0, 0)
    pair.wait()
    x_ref[half_rows(mc), :] = x_ref[half_rows(mc), :] + pair_ref[...]

    for i in range(PARTS):
        for j, (dx, dy) in enumerate(plane):
            q = plane_peer(dx, dy)
            remote(
                x_ref.at[slab_rows(mc, q), part(i)], plane_ref.at[i, j], plane_s.at[i], plane_r.at[i], at(q, mc, mz)
            ).start()

    def plane_all(i, send, recv):
        return remote(plane_ref.at[i], plane_ref.at[i], send.at[i], recv.at[i], at(mq, other, mz))

    def line_all(i):
        most = line_ref.at[i, pl.ds(0, nz - 1)]
        return remote(most, most, line_s.at[i], line_r.at[i], at(mq, other, mz))

    m1_ref[...] = contract(s_ref[...], s_ref[...], 0, 0)
    steps = rank // B
    cut1, cut2 = steps * CUT1 // 16, steps * CUT2 // 16
    factor_steps(m1_ref, 0, cut1)
    for i in range(PARTS):
        plane_all(i, plane_s, plane_r).wait_recv()
        total = x_ref[slab_rows(mc, mq), part(i)]
        for j in range(len(plane)):
            total = total + plane_ref[i, j]
        line_ref[i, mz] = total
        own = line_ref.at[i, mz]
        for dz in line:
            remote(own, own, line_s.at[i], line_r.at[i], at(mq, mc, (mz + dz) % nz)).start()
    factor_steps(m1_ref, cut1, cut2)
    for i in range(PARTS):
        line_all(i).wait_recv()
        full_ref[slab_rows(mc, mq), part(i)] = functools.reduce(jnp.add, [line_ref[i, z] for z in range(nz)])
        slab = full_ref.at[slab_rows(mc, mq), part(i)]
        for dx, dy in plane:
            remote(slab, slab, back_s.at[i], back_r.at[i], at(plane_peer(dx, dy), mc, mz)).start()
    factor_steps(m1_ref, cut2, steps)
    energy_all = jnp.sum(z_ref[...] * z_ref[...])

    def forward(i):
        block = full_ref.at[half_rows(mc), part(i)]
        return remote(block, block, fw_s.at[i], fw_r.at[i], at(mq, other, mz))

    for i in range(PARTS + 1):
        if i < PARTS:
            plane_all(i, back_s, back_r).wait_recv()
            forward(i).start()
        if i > 0:
            forward(i - 1).wait_recv()
            part_ref[...] = contract(m1_ref[...], full_ref[:, part(i - 1)], 1, 0)
            square = contract(part_ref[...], part_ref[...], 1, 1)
            m2_ref[...] = square if i == 1 else m2_ref[...] + square
            term = contract(z_ref[:, part(i - 1)], part_ref[...], 1, 1)
            w_ref[...] = term if i == 1 else w_ref[...] + term

    factor_steps(m2_ref, 0, steps)
    compressed = contract(w_ref[...], m2_ref[...], 1, 1)
    c_ref[...] = compressed
    energy_kept = jnp.sum(compressed * compressed)

    lane = lax.broadcasted_iota(jnp.int32, (1, 128), 1)
    e_ref[...] = jnp.where(lane == 0, energy_kept, jnp.where(lane == 1, energy_all, 0.0))
    ep_ref[mq] = e_ref[...]
    first = []
    for j, (dx, dy) in enumerate(plane):
        first.append(remote(e_ref, ep_ref.at[mq], ep_s.at[j], ep_r.at[j], at(plane_peer(dx, dy), mc, mz)))
        first[-1].start()
    for copy in first:
        copy.wait()
    e_ref[...] = functools.reduce(jnp.add, [ep_ref[q] for q in range(nq)])
    spot = mz * 2 + mc
    eq_ref[spot] = e_ref[...]
    second = []
    for j, (dz, dc) in enumerate([(dz, dc) for dc in range(2) for dz in [*line, 0] if dz or dc]):
        second.append(
            remote(e_ref, eq_ref.at[spot], eq_s.at[j], eq_r.at[j], at(mq, (mc + dc) % 2, (mz + dz) % nz))
        )
        second[-1].start()
    for i in range(PARTS):
        plane_all(i, plane_s, plane_r).wait_send()
        line_all(i).wait_send()
        plane_all(i, back_s, back_r).wait_send()
        forward(i).wait_send()
    for copy in second:
        copy.wait()
    sums = functools.reduce(jnp.add, [eq_ref[i] for i in range(2 * nz)])
    tail_ref[...] = 1.0 - sums[:, 0:1] / sums[:, 1:2]


def local(sizes, factor, start_block):
    nx, ny, nz = sizes
    nq = nx * ny
    depth, rank = start_block.shape
    half = rank // 2
    rows, cols = half // nq, depth // PARTS
    vmem = pl.BlockSpec(memory_space=pltpu.VMEM)
    hbm = pl.BlockSpec(memory_space=pltpu.HBM)
    dma = pltpu.SemaphoreType.DMA
    compressed, tail = pl.pallas_call(
        functools.partial(kernel, sizes),
        out_shape=(
            jax.ShapeDtypeStruct((factor.shape[0], rank), F32),
            jax.ShapeDtypeStruct((1, 1), F32),
        ),
        in_specs=[hbm, hbm],
        out_specs=(vmem, vmem),
        scratch_shapes=[
            pltpu.VMEM(factor.shape, F32),
            pltpu.VMEM(start_block.shape, F32),
            pltpu.VMEM((factor.shape[0], rank), F32),
            pltpu.VMEM((rank, depth), F32),
            pltpu.VMEM((half, depth), F32),
            pltpu.VMEM((PARTS, nq - 1, rows, cols), F32),
            pltpu.VMEM((PARTS, nz, rows, cols), F32),
            pltpu.VMEM((rank, depth), F32),
            pltpu.VMEM((rank, cols), F32),
            pltpu.VMEM((rank, rank), F32),
            pltpu.VMEM((rank, rank), F32),
            pltpu.VMEM((1, 128), F32),
            pltpu.VMEM((nq, 1, 128), F32),
            pltpu.VMEM((2 * nz, 1, 128), F32),
            dma((PARTS,)),
            dma((PARTS,)),
            dma,
            dma,
            *[dma((PARTS,)) for _ in range(8)],
            dma((nq - 1,)),
            dma((nq - 1,)),
            dma((2 * nz - 1,)),
            dma((2 * nz - 1,)),
        ],
        compiler_params=pltpu.CompilerParams(
            collective_id=0, has_side_effects=True, vmem_limit_bytes=40 * 2**20
        ),
    )(factor, start_block)
    return compressed, tail[0, 0]


def solution(mesh):
    side = math.isqrt(mesh.shape["rows"] // 2)
    sizes = (side, side, mesh.shape["grp"])
    return jax.shard_map(
        functools.partial(local, sizes),
        mesh=mesh,
        in_specs=(P(AXES, None), P()),
        out_specs=(P(AXES, None), P()),
        check_vma=False,
    )
```

```python
import functools
import math

import jax
import jax.numpy as jnp
from jax import lax
from jax.experimental import pallas as pl
from jax.experimental.pallas import tpu as pltpu
from jax.sharding import PartitionSpec as P

AXES = ("rows", "grp")
HI = lax.Precision.HIGHEST
B = 16
F32 = jnp.float32
PARTS = 4
VMEM_GRANT = 56_000_000
CUT1, CUT2 = 7, 11


def contract(a, b, da, db):
    return lax.dot_general(a, b, (((da,), (db,)), ((), ())), precision=HI, preferred_element_type=F32)


def contract3(a, b, da, db):
    def term(x, y):
        return lax.dot_general(x, y, (((da,), (db,)), ((), ())), preferred_element_type=F32)

    a1, b1 = a.astype(jnp.bfloat16), b.astype(jnp.bfloat16)
    a2, b2 = (a - a1.astype(F32)).astype(jnp.bfloat16), (b - b1.astype(F32)).astype(jnp.bfloat16)
    return term(a1, b1) + (term(a1, b2) + term(a2, b1))


def split3(x):
    a = x.astype(jnp.bfloat16).astype(F32)
    rest = x - a
    b = rest.astype(jnp.bfloat16).astype(F32)
    return a, b, (rest - b).astype(jnp.bfloat16).astype(F32)


def factor_step(m_ref, k):
    n = m_ref.shape[1]
    per = 128 // B
    row0 = pl.multiple_of(k * B, B)
    half = pl.multiple_of((k // per) * 128, 128)
    lane0 = (k % per) * B
    rows8 = lax.broadcasted_iota(jnp.int32, (8, 128), 0)
    diag = [m_ref[pl.ds(row0 + 8 * g, 8), pl.ds(half, 128)] for g in range(2)]
    column = {}
    for c in range(B):
        idx = jnp.full((8, 128), lane0 + c, jnp.int32)
        for g in range(2):
            if 8 * g + 8 > c:
                column[c, g] = jnp.take_along_axis(diag[g], idx, axis=1)
    lanes = lax.broadcasted_iota(jnp.int32, (8, n), 1) - k * B
    in_block = (lanes >= 0) & (lanes < B)
    wide = []
    for g in range(2):
        unit = jnp.where(lanes == 8 * g + lax.broadcasted_iota(jnp.int32, (8, n), 0), 1.0, 0.0)
        wide.append(jnp.where(in_block, unit, m_ref[pl.ds(row0 + 8 * g, 8), :]))
    pivots = [jnp.ones((8, 128), F32) for _ in range(2)]
    for c in range(B):
        gc, rc = divmod(c, 8)
        pivot = jnp.broadcast_to(column[c, gc][rc : rc + 1, :], (8, 128))
        pivots[gc] = jnp.where(rows8 == rc, pivot, pivots[gc])
        scale = 1.0 / pivot
        mult = {g: column[c, g] * scale for g in range(gc, 2)}
        mult[gc] = jnp.where(rows8 > rc, mult[gc], 0.0)
        pivot_row = jnp.broadcast_to(wide[gc][rc : rc + 1, :], (8, n))
        for d in range(c + 1, B):
            gd, rd = divmod(d, 8)
            entry = jnp.broadcast_to(column[c, gd][rd : rd + 1, :], (8, 128))
            for g in range(gd, 2):
                column[d, g] = column[d, g] - mult[g] * entry
        for g in range(gc, 2):
            wide[g] = wide[g] - jnp.tile(mult[g], (1, n // 128)) * pivot_row
    final = []
    for g in range(2):
        s = lax.rsqrt(pivots[g])
        s = s * (1.5 - 0.5 * pivots[g] * s * s)
        final.append(wide[g] * jnp.tile(s, (1, n // 128)))
    u = jnp.concatenate(final, axis=0)
    a, b, c = split3(u)
    right = jnp.concatenate([a, b, a, c, b, a], axis=0).astype(jnp.bfloat16)
    later = lax.broadcasted_iota(jnp.int32, (B, n), 1) >= (k + 1) * B
    a, b, c = (jnp.where(later, t, 0.0) for t in (a, b, c))
    left = jnp.concatenate([a, a, b, a, b, c], axis=0).T.astype(jnp.bfloat16)
    update = jnp.dot(left, right, preferred_element_type=F32)
    cols = lax.broadcasted_iota(jnp.int32, (n, n), 1) - k * B
    m_ref[...] = jnp.where((cols >= 0) & (cols < B), 0.0, m_ref[...]) - update
    m_ref[pl.ds(row0, B), :] = u


def factor_steps(m_ref, lo, hi):
    def body(k, carry):
        factor_step(m_ref, k)
        return carry

    lax.fori_loop(lo, hi, body, 0)


def kernel(
    sizes,
    z_hbm,
    s_hbm,
    c_ref,
    tail_ref,
    z_ref,
    s_ref,
    w_ref,
    x_ref,
    pair_ref,
    plane_ref,
    line_ref,
    full_ref,
    part_ref,
    m1_ref,
    m2_ref,
    e_ref,
    ep_ref,
    eq_ref,
    *sems,
):
    nx, ny, nz = sizes
    (z_in, s_in, pair_s, pair_r, plane_s, plane_r, line_s, line_r, back_s, back_r, fw_s, fw_r, ep_s, ep_r, eq_s, eq_r) = sems
    nq = nx * ny
    rank, depth = s_ref.shape[1], s_ref.shape[0]
    half = rank // 2
    rows, cols = half // nq, depth // PARTS
    me = lax.axis_index("rows")
    mz = lax.axis_index("grp")
    mc = me % 2
    mq = me // 2
    mx, my = mq // ny, mq % ny

    def at(q, c, z):
        return {"rows": q * 2 + c, "grp": z}

    def plane_peer(dx, dy):
        return ((mx + dx) % nx) * ny + (my + dy) % ny

    far = lambda d, n: min(d, n - d)
    plane = [(dx, dy) for dx in range(nx) for dy in range(ny) if dx or dy]
    plane.sort(key=lambda d: (-far(d[0], nx) - far(d[1], ny), d))
    line = sorted(range(1, nz), key=lambda d: (-far(d, nz), d))
    other = 1 - mc

    def part(i):
        return pl.ds(i * cols, cols)

    loads = []
    for i in range(PARTS):
        loads.append(pltpu.make_async_copy(z_hbm.at[:, part(i)], z_ref.at[:, part(i)], z_in.at[i]))
        loads.append(pltpu.make_async_copy(s_hbm.at[part(i), :], s_ref.at[part(i), :], s_in.at[i]))
    for copy in loads:
        copy.start()

    barrier = pltpu.get_barrier_semaphore()
    greet = [at(mq, other, mz)]
    greet += [at(plane_peer(dx, dy), mc, mz) for dx, dy in plane]
    greet += [at(mq, mc, (mz + dz) % nz) for dz in line]
    greet += [at(mq, other, (mz + dz) % nz) for dz in line]
    for device in greet:
        pl.semaphore_signal(barrier, inc=1, device_id=device, device_id_type=pl.DeviceIdType.MESH)

    def remote(src, dst, send, recv, device):
        return pltpu.make_async_remote_copy(
            src_ref=src, dst_ref=dst, send_sem=send, recv_sem=recv, device_id=device, device_id_type=pl.DeviceIdType.MESH
        )

    def half_rows(c):
        return pl.ds(pl.multiple_of(c * half, half), half)

    def slab_rows(c, q):
        return pl.ds(pl.multiple_of(c * half + q * rows, rows), rows)

    for i in range(PARTS):
        loads[2 * i].wait()
        loads[2 * i + 1].wait()
        term = contract3(z_ref[:, part(i)], s_ref[part(i), :], 1, 0)
        w_ref[...] = term if i == 0 else w_ref[...] + term
    x_ref[half_rows(other), :] = contract3(w_ref[:, half_rows(other)].T, z_ref[...], 1, 0)
    pl.semaphore_wait(barrier, len(greet))
    pair = remote(x_ref.at[half_rows(other), :], pair_ref, pair_s, pair_r, at(mq, other, mz))
    pair.start()
    x_ref[half_rows(mc), :] = contract3(w_ref[:, half_rows(mc)].T, z_ref[...], 1, 0)
    pair.wait()
    x_ref[half_rows(mc), :] = x_ref[half_rows(mc), :] + pair_ref[...]

    for i in range(PARTS):
        for j, (dx, dy) in enumerate(plane):
            q = plane_peer(dx, dy)
            remote(
                x_ref.at[slab_rows(mc, q), part(i)], plane_ref.at[i, j], plane_s.at[i], plane_r.at[i], at(q, mc, mz)
            ).start()

    def plane_all(i, send, recv):
        return remote(plane_ref.at[i], plane_ref.at[i], send.at[i], recv.at[i], at(mq, other, mz))

    def line_all(i):
        most = line_ref.at[i, pl.ds(0, nz - 1)]
        return remote(most, most, line_s.at[i], line_r.at[i], at(mq, other, mz))

    m1_ref[...] = contract(s_ref[...], s_ref[...], 0, 0)
    steps = rank // B
    cut1, cut2 = steps * CUT1 // 16, steps * CUT2 // 16
    factor_steps(m1_ref, 0, cut1)
    for i in range(PARTS):
        plane_all(i, plane_s, plane_r).wait_recv()
        total = x_ref[slab_rows(mc, mq), part(i)]
        for j in range(len(plane)):
            total = total + plane_ref[i, j]
        line_ref[i, mz] = total
        own = line_ref.at[i, mz]
        for dz in line:
            remote(own, own, line_s.at[i], line_r.at[i], at(mq, mc, (mz + dz) % nz)).start()
    factor_steps(m1_ref, cut1, cut2)
    for i in range(PARTS):
        line_all(i).wait_recv()
        full_ref[slab_rows(mc, mq), part(i)] = functools.reduce(jnp.add, [line_ref[i, z] for z in range(nz)])
        slab = full_ref.at[slab_rows(mc, mq), part(i)]
        for dx, dy in plane:
            remote(slab, slab, back_s.at[i], back_r.at[i], at(plane_peer(dx, dy), mc, mz)).start()
    factor_steps(m1_ref, cut2, steps)
    energy_all = jnp.sum(z_ref[...] * z_ref[...])

    def forward(i):
        block = full_ref.at[half_rows(mc), part(i)]
        return remote(block, block, fw_s.at[i], fw_r.at[i], at(mq, other, mz))

    for i in range(PARTS + 1):
        if i < PARTS:
            plane_all(i, back_s, back_r).wait_recv()
            forward(i).start()
        if i > 0:
            forward(i - 1).wait_recv()
            part_ref[...] = contract3(m1_ref[...], full_ref[:, part(i - 1)], 1, 0)
            square = contract(part_ref[...], part_ref[...], 1, 1)
            m2_ref[...] = square if i == 1 else m2_ref[...] + square
            term = contract3(z_ref[:, part(i - 1)], part_ref[...], 1, 1)
            w_ref[...] = term if i == 1 else w_ref[...] + term

    factor_steps(m2_ref, 0, steps)
    compressed = contract3(w_ref[...], m2_ref[...], 1, 1)
    c_ref[...] = compressed
    energy_kept = jnp.sum(compressed * compressed)

    lane = lax.broadcasted_iota(jnp.int32, (1, 128), 1)
    e_ref[...] = jnp.where(lane == 0, energy_kept, jnp.where(lane == 1, energy_all, 0.0))
    ep_ref[mq] = e_ref[...]
    first = []
    for j, (dx, dy) in enumerate(plane):
        first.append(remote(e_ref, ep_ref.at[mq], ep_s.at[j], ep_r.at[j], at(plane_peer(dx, dy), mc, mz)))
        first[-1].start()
    for copy in first:
        copy.wait()
    e_ref[...] = functools.reduce(jnp.add, [ep_ref[q] for q in range(nq)])
    spot = mz * 2 + mc
    eq_ref[spot] = e_ref[...]
    second = []
    for j, (dz, dc) in enumerate([(dz, dc) for dc in range(2) for dz in [*line, 0] if dz or dc]):
        second.append(
            remote(e_ref, eq_ref.at[spot], eq_s.at[j], eq_r.at[j], at(mq, (mc + dc) % 2, (mz + dz) % nz))
        )
        second[-1].start()
    for i in range(PARTS):
        plane_all(i, plane_s, plane_r).wait_send()
        line_all(i).wait_send()
        plane_all(i, back_s, back_r).wait_send()
        forward(i).wait_send()
    for copy in second:
        copy.wait()
    sums = functools.reduce(jnp.add, [eq_ref[i] for i in range(2 * nz)])
    tail_ref[...] = 1.0 - sums[:, 0:1] / sums[:, 1:2]


def local(sizes, factor, start_block):
    nx, ny, nz = sizes
    nq = nx * ny
    depth, rank = start_block.shape
    half = rank // 2
    rows, cols = half // nq, depth // PARTS
    vmem = pl.BlockSpec(memory_space=pltpu.VMEM)
    hbm = pl.BlockSpec(memory_space=pltpu.HBM)
    dma = pltpu.SemaphoreType.DMA
    compressed, tail = pl.pallas_call(
        functools.partial(kernel, sizes),
        out_shape=(
            jax.ShapeDtypeStruct((factor.shape[0], rank), F32),
            jax.ShapeDtypeStruct((1, 1), F32),
        ),
        in_specs=[hbm, hbm],
        out_specs=(vmem, vmem),
        scratch_shapes=[
            pltpu.VMEM(factor.shape, F32),
            pltpu.VMEM(start_block.shape, F32),
            pltpu.VMEM((factor.shape[0], rank), F32),
            pltpu.VMEM((rank, depth), F32),
            pltpu.VMEM((half, depth), F32),
            pltpu.VMEM((PARTS, nq - 1, rows, cols), F32),
            pltpu.VMEM((PARTS, nz, rows, cols), F32),
            pltpu.VMEM((rank, depth), F32),
            pltpu.VMEM((rank, cols), F32),
            pltpu.VMEM((rank, rank), F32),
            pltpu.VMEM((rank, rank), F32),
            pltpu.VMEM((1, 128), F32),
            pltpu.VMEM((nq, 1, 128), F32),
            pltpu.VMEM((2 * nz, 1, 128), F32),
            dma((PARTS,)),
            dma((PARTS,)),
            dma,
            dma,
            *[dma((PARTS,)) for _ in range(8)],
            dma((nq - 1,)),
            dma((nq - 1,)),
            dma((2 * nz - 1,)),
            dma((2 * nz - 1,)),
        ],
        compiler_params=pltpu.CompilerParams(
            collective_id=0, has_side_effects=True, vmem_limit_bytes=VMEM_GRANT
        ),
    )(factor, start_block)
    return compressed, tail[0, 0]


def solution(mesh):
    side = math.isqrt(mesh.shape["rows"] // 2)
    sizes = (side, side, mesh.shape["grp"])
    return jax.shard_map(
        functools.partial(local, sizes),
        mesh=mesh,
        in_specs=(P(AXES, None), P()),
        out_specs=(P(AXES, None), P()),
        check_vma=False,
    )
```

```python
import functools
import math

import jax
import jax.numpy as jnp
from jax import lax
from jax.experimental import pallas as pl
from jax.experimental.pallas import tpu as pltpu
from jax.sharding import PartitionSpec as P

AXES = ("rows", "grp")
HI = lax.Precision.HIGHEST
B = 16
F32 = jnp.float32
PARTS = 4
VMEM_GRANT = 56_000_000
ORDER = (0, 2, 1, 3)
CUTS = (0, 6, 8, 13, 16)


def contract(a, b, da, db):
    return lax.dot_general(a, b, (((da,), (db,)), ((), ())), precision=HI, preferred_element_type=F32)


def contract3(a, b, da, db):
    def term(x, y):
        return lax.dot_general(x, y, (((da,), (db,)), ((), ())), preferred_element_type=F32)

    a1, b1 = a.astype(jnp.bfloat16), b.astype(jnp.bfloat16)
    a2, b2 = (a - a1.astype(F32)).astype(jnp.bfloat16), (b - b1.astype(F32)).astype(jnp.bfloat16)
    return term(a1, b1) + (term(a1, b2) + term(a2, b1))


def split3(x):
    a = x.astype(jnp.bfloat16).astype(F32)
    rest = x - a
    b = rest.astype(jnp.bfloat16).astype(F32)
    return a, b, (rest - b).astype(jnp.bfloat16).astype(F32)


def factor_step(m_ref, k):
    n = m_ref.shape[1]
    per = 128 // B
    row0 = pl.multiple_of(k * B, B)
    half = pl.multiple_of((k // per) * 128, 128)
    lane0 = (k % per) * B
    rows8 = lax.broadcasted_iota(jnp.int32, (8, 128), 0)
    diag = [m_ref[pl.ds(row0 + 8 * g, 8), pl.ds(half, 128)] for g in range(2)]
    column = {}
    for c in range(B):
        idx = jnp.full((8, 128), lane0 + c, jnp.int32)
        for g in range(2):
            if 8 * g + 8 > c:
                column[c, g] = jnp.take_along_axis(diag[g], idx, axis=1)
    lanes = lax.broadcasted_iota(jnp.int32, (8, n), 1) - k * B
    in_block = (lanes >= 0) & (lanes < B)
    wide = []
    for g in range(2):
        unit = jnp.where(lanes == 8 * g + lax.broadcasted_iota(jnp.int32, (8, n), 0), 1.0, 0.0)
        wide.append(jnp.where(in_block, unit, m_ref[pl.ds(row0 + 8 * g, 8), :]))
    pivots = [jnp.ones((8, 128), F32) for _ in range(2)]
    for c in range(B):
        gc, rc = divmod(c, 8)
        pivot = jnp.broadcast_to(column[c, gc][rc : rc + 1, :], (8, 128))
        pivots[gc] = jnp.where(rows8 == rc, pivot, pivots[gc])
        scale = 1.0 / pivot
        mult = {g: column[c, g] * scale for g in range(gc, 2)}
        mult[gc] = jnp.where(rows8 > rc, mult[gc], 0.0)
        pivot_row = jnp.broadcast_to(wide[gc][rc : rc + 1, :], (8, n))
        for d in range(c + 1, B):
            gd, rd = divmod(d, 8)
            entry = jnp.broadcast_to(column[c, gd][rd : rd + 1, :], (8, 128))
            for g in range(gd, 2):
                column[d, g] = column[d, g] - mult[g] * entry
        for g in range(gc, 2):
            wide[g] = wide[g] - jnp.tile(mult[g], (1, n // 128)) * pivot_row
    final = []
    for g in range(2):
        s = lax.rsqrt(pivots[g])
        s = s * (1.5 - 0.5 * pivots[g] * s * s)
        final.append(wide[g] * jnp.tile(s, (1, n // 128)))
    u = jnp.concatenate(final, axis=0)
    a, b, c = split3(u)
    right = jnp.concatenate([a, b, a, c, b, a], axis=0).astype(jnp.bfloat16)
    later = lax.broadcasted_iota(jnp.int32, (B, n), 1) >= (k + 1) * B
    a, b, c = (jnp.where(later, t, 0.0) for t in (a, b, c))
    left = jnp.concatenate([a, a, b, a, b, c], axis=0).T.astype(jnp.bfloat16)
    update = jnp.dot(left, right, preferred_element_type=F32)
    cols = lax.broadcasted_iota(jnp.int32, (n, n), 1) - k * B
    m_ref[...] = jnp.where((cols >= 0) & (cols < B), 0.0, m_ref[...]) - update
    m_ref[pl.ds(row0, B), :] = u


def factor_steps(m_ref, lo, hi):
    def body(k, carry):
        factor_step(m_ref, k)
        return carry

    lax.fori_loop(lo, hi, body, 0)


def kernel(
    sizes,
    z_hbm,
    s_hbm,
    c_ref,
    tail_ref,
    z_ref,
    s_ref,
    w_ref,
    x_ref,
    pair_ref,
    near_ref,
    mid_ref,
    next_ref,
    line_ref,
    most_ref,
    full_ref,
    part_ref,
    m1_ref,
    m2_ref,
    e_ref,
    ep_ref,
    eq_ref,
    *sems,
):
    nx, ny, nz = sizes
    (z_in, s_in, pair_s, pair_r, near_s, near_r, next_s, next_r, line_s, line_r, back_s, back_r, fw_s, fw_r, ep_s, ep_r, eq_s, eq_r) = sems
    nq = nx * ny
    rank, depth = s_ref.shape[1], s_ref.shape[0]
    half = rank // 2
    rows, cols = half // nq, depth // PARTS
    me = lax.axis_index("rows")
    mz = lax.axis_index("grp")
    mc = me % 2
    mq = me // 2
    mx, my = mq // ny, mq % ny

    def at(q, c, z):
        return {"rows": q * 2 + c, "grp": z}

    def plane_peer(dx, dy):
        return ((mx + dx) % nx) * ny + (my + dy) % ny

    far = lambda d, n: min(d, n - d)
    plane = [(dx, dy) for dx in range(nx) for dy in range(ny) if dx or dy]
    plane.sort(key=lambda d: (-far(d[0], nx) - far(d[1], ny), d))
    line = sorted(range(1, nz), key=lambda d: (-far(d, nz), d))
    other = 1 - mc
    distances = sorted(range(1, nx), key=lambda d: (-far(d, nx), d))

    def part(i):
        return pl.ds(i * cols, cols)

    loads = []
    for i in range(PARTS):
        loads.append(pltpu.make_async_copy(z_hbm.at[:, part(i)], z_ref.at[:, part(i)], z_in.at[i]))
        loads.append(pltpu.make_async_copy(s_hbm.at[part(i), :], s_ref.at[part(i), :], s_in.at[i]))
    for copy in loads:
        copy.start()

    barrier = pltpu.get_barrier_semaphore()
    greet = [at(mq, other, mz)]
    greet += [at(plane_peer(dx, dy), mc, mz) for dx, dy in plane]
    greet += [at(mq, mc, (mz + dz) % nz) for dz in line]
    greet += [at(mq, other, (mz + dz) % nz) for dz in line]
    for device in greet:
        pl.semaphore_signal(barrier, inc=1, device_id=device, device_id_type=pl.DeviceIdType.MESH)

    def remote(src, dst, send, recv, device):
        return pltpu.make_async_remote_copy(
            src_ref=src, dst_ref=dst, send_sem=send, recv_sem=recv, device_id=device, device_id_type=pl.DeviceIdType.MESH
        )

    def half_rows(c):
        return pl.ds(pl.multiple_of(c * half, half), half)

    def slab_rows(c, q):
        return pl.ds(pl.multiple_of(c * half + q * rows, rows), rows)

    def image_rows(c):
        return contract3(w_ref[:, half_rows(c)].T, z_ref[...], 1, 0).reshape(nx, ny, rows, depth)

    for i in range(PARTS):
        loads[2 * i].wait()
        loads[2 * i + 1].wait()
        term = contract3(z_ref[:, part(i)], s_ref[part(i), :], 1, 0)
        w_ref[...] = term if i == 0 else w_ref[...] + term
    x_ref[other] = image_rows(other)
    pl.semaphore_wait(barrier, len(greet))
    pair = remote(x_ref.at[other], pair_ref, pair_s, pair_r, at(mq, other, mz))
    pair.start()
    x_ref[mc] = image_rows(mc)
    pair.wait()
    x_ref[mc] = x_ref[mc] + pair_ref[...]

    def x_first(i):
        return i < PARTS // 2

    def terms(i, tx, ty):
        return x_ref.at[mc, tx, :, :, part(i)] if x_first(i) else x_ref.at[mc, :, ty, :, part(i)]

    for i in ORDER:
        for j, d in enumerate(distances):
            tx, ty = ((mx + d) % nx, my) if x_first(i) else (mx, (my + d) % ny)
            remote(terms(i, tx, ty), near_ref.at[i, j], near_s.at[i], near_r.at[i], at(tx * ny + ty, mc, mz)).start()

    def everything(ref, i, send, recv):
        return remote(ref.at[i], ref.at[i], send.at[i], recv.at[i], at(mq, other, mz))

    def line_all(i):
        most = line_ref.at[i, pl.ds(0, nz - 1)]
        return remote(most, most, line_s.at[i], line_r.at[i], at(mq, other, mz))

    m1_ref[...] = contract(s_ref[...], s_ref[...], 0, 0)
    steps = rank // B
    cuts = [steps * cut // 16 for cut in CUTS]
    factor_steps(m1_ref, cuts[0], cuts[1])
    for i in ORDER:
        everything(near_ref, i, near_s, near_r).wait_recv()
        total = terms(i, mx, my)[...]
        for j in range(len(distances)):
            total = total + near_ref[i, j]
        mid_ref[i] = total
        for j, d in enumerate(distances):
            tx, ty = (mx, (my + d) % ny) if x_first(i) else ((mx + d) % nx, my)
            block = mid_ref.at[i, ty if x_first(i) else tx]
            remote(block, next_ref.at[i, j], next_s.at[i], next_r.at[i], at(tx * ny + ty, mc, mz)).start()
    factor_steps(m1_ref, cuts[1], cuts[2])
    for i in ORDER:
        everything(next_ref, i, next_s, next_r).wait_recv()
        total = mid_ref[i, my if x_first(i) else mx]
        for j in range(len(distances)):
            total = total + next_ref[i, j]
        line_ref[i, mz] = total
        own = line_ref.at[i, mz]
        for dz in line:
            remote(own, own, line_s.at[i], line_r.at[i], at(mq, mc, (mz + dz) % nz)).start()
    factor_steps(m1_ref, cuts[2], cuts[3])
    for i in ORDER:
        line_all(i).wait_recv()
        full_ref[slab_rows(mc, mq), part(i)] = functools.reduce(jnp.add, [line_ref[i, z] for z in range(nz)])
        slab = full_ref.at[slab_rows(mc, mq), part(i)]
        for dx, dy in plane:
            remote(slab, slab, back_s.at[i], back_r.at[i], at(plane_peer(dx, dy), mc, mz)).start()
    factor_steps(m1_ref, cuts[3], cuts[4])
    energy_all = jnp.sum(z_ref[...] * z_ref[...])

    def forward(i):
        block = full_ref.at[half_rows(mc), part(i)]
        return remote(block, block, fw_s.at[i], fw_r.at[i], at(mq, other, mz))

    def gathered(i):
        most = most_ref.at[pl.ds(0, nq - 1)]
        return remote(most, most, back_s.at[i], back_r.at[i], at(mq, other, mz))

    for place in range(PARTS + 1):
        if place < PARTS:
            i = ORDER[place]
            gathered(i).wait_recv()
            forward(i).start()
        if place > 0:
            i = ORDER[place - 1]
            forward(i).wait_recv()
            part_ref[...] = contract3(m1_ref[...], full_ref[:, part(i)], 1, 0)
            square = contract(part_ref[...], part_ref[...], 1, 1)
            m2_ref[...] = square if place == 1 else m2_ref[...] + square
            term = contract3(z_ref[:, part(i)], part_ref[...], 1, 1)
            w_ref[...] = term if place == 1 else w_ref[...] + term

    factor_steps(m2_ref, 0, steps)
    compressed = contract3(w_ref[...], m2_ref[...], 1, 1)
    c_ref[...] = compressed
    energy_kept = jnp.sum(compressed * compressed)

    lane = lax.broadcasted_iota(jnp.int32, (1, 128), 1)
    e_ref[...] = jnp.where(lane == 0, energy_kept, jnp.where(lane == 1, energy_all, 0.0))
    ep_ref[mq] = e_ref[...]
    first = []
    for j, (dx, dy) in enumerate(plane):
        first.append(remote(e_ref, ep_ref.at[mq], ep_s.at[j], ep_r.at[j], at(plane_peer(dx, dy), mc, mz)))
        first[-1].start()
    for copy in first:
        copy.wait()
    e_ref[...] = functools.reduce(jnp.add, [ep_ref[q] for q in range(nq)])
    spot = mz * 2 + mc
    eq_ref[spot] = e_ref[...]
    second = []
    for j, (dz, dc) in enumerate([(dz, dc) for dc in range(2) for dz in [*line, 0] if dz or dc]):
        second.append(
            remote(e_ref, eq_ref.at[spot], eq_s.at[j], eq_r.at[j], at(mq, (mc + dc) % 2, (mz + dz) % nz))
        )
        second[-1].start()
    for i in range(PARTS):
        everything(near_ref, i, near_s, near_r).wait_send()
        everything(next_ref, i, next_s, next_r).wait_send()
        line_all(i).wait_send()
        gathered(i).wait_send()
        forward(i).wait_send()
    for copy in second:
        copy.wait()
    sums = functools.reduce(jnp.add, [eq_ref[i] for i in range(2 * nz)])
    tail_ref[...] = 1.0 - sums[:, 0:1] / sums[:, 1:2]


def local(sizes, factor, start_block):
    nx, ny, nz = sizes
    nq = nx * ny
    depth, rank = start_block.shape
    half = rank // 2
    rows, cols = half // nq, depth // PARTS
    vmem = pl.BlockSpec(memory_space=pltpu.VMEM)
    hbm = pl.BlockSpec(memory_space=pltpu.HBM)
    dma = pltpu.SemaphoreType.DMA
    compressed, tail = pl.pallas_call(
        functools.partial(kernel, sizes),
        out_shape=(
            jax.ShapeDtypeStruct((factor.shape[0], rank), F32),
            jax.ShapeDtypeStruct((1, 1), F32),
        ),
        in_specs=[hbm, hbm],
        out_specs=(vmem, vmem),
        scratch_shapes=[
            pltpu.VMEM(factor.shape, F32),
            pltpu.VMEM(start_block.shape, F32),
            pltpu.VMEM((factor.shape[0], rank), F32),
            pltpu.VMEM((2, nx, ny, rows, depth), F32),
            pltpu.VMEM((nx, ny, rows, depth), F32),
            pltpu.VMEM((PARTS, nx - 1, nx, rows, cols), F32),
            pltpu.VMEM((PARTS, nx, rows, cols), F32),
            pltpu.VMEM((PARTS, nx - 1, rows, cols), F32),
            pltpu.VMEM((PARTS, nz, rows, cols), F32),
            pltpu.VMEM((nq, rows, cols), F32),
            pltpu.VMEM((rank, depth), F32),
            pltpu.VMEM((rank, cols), F32),
            pltpu.VMEM((rank, rank), F32),
            pltpu.VMEM((rank, rank), F32),
            pltpu.VMEM((1, 128), F32),
            pltpu.VMEM((nq, 1, 128), F32),
            pltpu.VMEM((2 * nz, 1, 128), F32),
            dma((PARTS,)),
            dma((PARTS,)),
            dma,
            dma,
            *[dma((PARTS,)) for _ in range(10)],
            dma((nq - 1,)),
            dma((nq - 1,)),
            dma((2 * nz - 1,)),
            dma((2 * nz - 1,)),
        ],
        compiler_params=pltpu.CompilerParams(
            collective_id=0, has_side_effects=True, vmem_limit_bytes=VMEM_GRANT
        ),
    )(factor, start_block)
    return compressed, tail[0, 0]


def solution(mesh):
    side = math.isqrt(mesh.shape["rows"] // 2)
    sizes = (side, side, mesh.shape["grp"])
    return jax.shard_map(
        functools.partial(local, sizes),
        mesh=mesh,
        in_specs=(P(AXES, None), P()),
        out_specs=(P(AXES, None), P()),
        check_vma=False,
    )
```

```python
import functools
import math

import jax
import jax.numpy as jnp
from jax import lax
from jax.experimental import pallas as pl
from jax.experimental.pallas import tpu as pltpu
from jax.sharding import PartitionSpec as P

AXES = ("rows", "grp")
HI = lax.Precision.HIGHEST
B = 16
PANEL1, PANEL2 = 32, 64
F32 = jnp.float32
PARTS = 4
VMEM_GRANT = 56_000_000
CUT1, CUT2 = 8, 12


def contract(a, b, da, db):
    return lax.dot_general(a, b, (((da,), (db,)), ((), ())), precision=HI, preferred_element_type=F32)


def split2(x):
    a = x.astype(jnp.bfloat16)
    return a, (x - a.astype(F32)).astype(jnp.bfloat16)


def product3(a, b, da, db):
    def term(x, y):
        return lax.dot_general(x, y, (((da,), (db,)), ((), ())), preferred_element_type=F32)

    return term(a[0], b[0]) + (term(a[0], b[1]) + term(a[1], b[0]))


def split3(x):
    a = x.astype(jnp.bfloat16).astype(F32)
    rest = x - a
    b = rest.astype(jnp.bfloat16).astype(F32)
    return a, b, (rest - b).astype(jnp.bfloat16).astype(F32)


def factor_step(m_ref, left_ref, right_ref, k):
    n = m_ref.shape[1]
    panel_rows = right_ref.shape[0] // 6
    row0 = pl.multiple_of(k * panel_rows, panel_rows)
    groups = panel_rows // 8
    rows8 = lax.broadcasted_iota(jnp.int32, (8, 128), 0)
    left, right = left_ref[...], right_ref[...]
    own = jnp.dot(left_ref[pl.ds(row0, panel_rows), :], right, preferred_element_type=F32)
    lanes = lax.broadcasted_iota(jnp.int32, (panel_rows, n), 1) - row0
    panel = jnp.where((lanes >= -panel_rows) & (lanes < 0), 0.0, m_ref[pl.ds(row0, panel_rows), :]) - own
    cols = lax.broadcasted_iota(jnp.int32, (n, n), 1) - row0
    update = jnp.dot(left, right, preferred_element_type=F32)
    below = lax.broadcasted_iota(jnp.int32, (n, n), 0) >= row0
    m_ref[...] = jnp.where(below & (cols >= -panel_rows) & (cols < 0), 0.0, m_ref[...]) - update
    wide = [panel[8 * g : 8 * g + 8] for g in range(groups)]
    pivots = [jnp.ones((8, 128), F32) for _ in range(groups)]
    lane8 = lanes[:8]
    place8 = lax.broadcasted_iota(jnp.int32, (8, n), 0)
    upper = row0 >= 128
    for b in range(panel_rows // B):
        first = b * B // 8
        lane0 = row0 % 128 + b * B
        column = {}
        for c in range(B):
            idx = jnp.full((8, 128), lane0 + c, jnp.int32)
            for g in range(first + c // 8, groups):
                column[c, g] = jnp.take_along_axis(jnp.where(upper, wide[g][:, 128:], wide[g][:, :128]), idx, axis=1)
        in_block = (lane8 >= b * B) & (lane8 < b * B + B)
        for g in range(first, groups):
            unit = jnp.where(lane8 == 8 * g + place8, 1.0, 0.0) if g < first + B // 8 else 0.0
            wide[g] = jnp.where(in_block, unit, wide[g])
        for c in range(B):
            gc, rc = first + c // 8, c % 8
            pivot = jnp.broadcast_to(column[c, gc][rc : rc + 1, :], (8, 128))
            pivots[gc] = jnp.where(rows8 == rc, pivot, pivots[gc])
            scale = 1.0 / pivot
            mult = {g: column[c, g] * scale for g in range(gc, groups)}
            mult[gc] = jnp.where(rows8 > rc, mult[gc], 0.0)
            pivot_row = jnp.broadcast_to(wide[gc][rc : rc + 1, :], (8, n))
            for d in range(c + 1, B):
                gd, rd = first + d // 8, d % 8
                entry = jnp.broadcast_to(column[c, gd][rd : rd + 1, :], (8, 128))
                for g in range(gd, groups):
                    column[d, g] = column[d, g] - mult[g] * entry
            for g in range(gc, groups):
                wide[g] = wide[g] - jnp.tile(mult[g], (1, n // 128)) * pivot_row
    final = []
    for g in range(groups):
        s = lax.rsqrt(pivots[g])
        s = s * (1.5 - 0.5 * pivots[g] * s * s)
        final.append(wide[g] * jnp.tile(s, (1, n // 128)))
    u = jnp.concatenate(final, axis=0)
    inside = lax.broadcasted_iota(jnp.int32, (panel_rows, n), 0)
    u = jnp.where((lanes < panel_rows) & (lanes > inside), 0.0, u)
    a, b, c = split3(u)
    right_ref[...] = jnp.concatenate([a, b, a, c, b, a], axis=0).astype(jnp.bfloat16)
    a, b, c = (jnp.where(lanes >= panel_rows, t, 0.0) for t in (a, b, c))
    left_ref[...] = jnp.concatenate([a, a, b, a, b, c], axis=0).T.astype(jnp.bfloat16)
    m_ref[pl.ds(row0, panel_rows), :] = u


def factor_steps(refs, lo, hi):
    m_ref, left_ref, right_ref = refs
    n = m_ref.shape[1]
    if lo == 0:
        left_ref[...] = jnp.zeros_like(left_ref)
        right_ref[...] = jnp.zeros_like(right_ref)

    def body(k, carry):
        factor_step(m_ref, left_ref, right_ref, k)
        return carry

    lax.fori_loop(lo, hi, body, 0)
    if hi == steps_of(refs):
        rows, cols = (lax.broadcasted_iota(jnp.int32, (n, n), d) for d in range(2))
        m_ref[...] = jnp.where(rows >= cols, m_ref[...], 0.0)


def steps_of(refs):
    return refs[0].shape[0] * 6 // refs[2].shape[0]


def kernel(
    sizes,
    z_hbm,
    s_hbm,
    c_ref,
    tail_ref,
    z_ref,
    s_ref,
    w_ref,
    x_ref,
    pair_ref,
    plane_ref,
    line_ref,
    full_ref,
    part_ref,
    z1_ref,
    z2_ref,
    m1_ref,
    left1_ref,
    right1_ref,
    m2_ref,
    left2_ref,
    right2_ref,
    e_ref,
    ep_ref,
    eq_ref,
    *sems,
):
    nx, ny, nz = sizes
    (z_in, s_in, pair_s, pair_r, plane_s, plane_r, line_s, line_r, back_s, back_r, fw_s, fw_r, ep_s, ep_r, eq_s, eq_r) = sems
    nq = nx * ny
    rank, depth = s_ref.shape[1], s_ref.shape[0]
    half = rank // 2
    rows, cols = half // nq, depth // PARTS
    me = lax.axis_index("rows")
    mz = lax.axis_index("grp")
    mc = me % 2
    mq = me // 2
    mx, my = mq // ny, mq % ny

    def at(q, c, z):
        return {"rows": q * 2 + c, "grp": z}

    def plane_peer(dx, dy):
        return ((mx + dx) % nx) * ny + (my + dy) % ny

    far = lambda d, n: min(d, n - d)
    plane = [(dx, dy) for dx in range(nx) for dy in range(ny) if dx or dy]
    plane.sort(key=lambda d: (-far(d[0], nx) - far(d[1], ny), d))
    line = sorted(range(1, nz), key=lambda d: (-far(d, nz), d))
    other = 1 - mc

    def part(i):
        return pl.ds(i * cols, cols)

    loads = []
    for i in range(PARTS):
        loads.append(pltpu.make_async_copy(z_hbm.at[:, part(i)], z_ref.at[:, part(i)], z_in.at[i]))
        loads.append(pltpu.make_async_copy(s_hbm.at[part(i), :], s_ref.at[part(i), :], s_in.at[i]))
    for copy in loads:
        copy.start()

    barrier = pltpu.get_barrier_semaphore()
    greet = [at(mq, other, mz)]
    greet += [at(plane_peer(dx, dy), mc, mz) for dx, dy in plane]
    greet += [at(mq, mc, (mz + dz) % nz) for dz in line]
    greet += [at(mq, other, (mz + dz) % nz) for dz in line]
    for device in greet:
        pl.semaphore_signal(barrier, inc=1, device_id=device, device_id_type=pl.DeviceIdType.MESH)

    def remote(src, dst, send, recv, device):
        return pltpu.make_async_remote_copy(
            src_ref=src, dst_ref=dst, send_sem=send, recv_sem=recv, device_id=device, device_id_type=pl.DeviceIdType.MESH
        )

    def half_rows(c):
        return pl.ds(pl.multiple_of(c * half, half), half)

    def slab_rows(c, q):
        return pl.ds(pl.multiple_of(c * half + q * rows, rows), rows)

    def halves(n):
        return slice(0, n // 2), slice(n // 2, n)

    def image_rows(c):
        rows_of_c = split2(w_ref[:, half_rows(c)].T)
        for h in halves(depth):
            x_ref[half_rows(c), h] = product3(rows_of_c, (z1_ref[:, h], z2_ref[:, h]), 1, 0)

    for i in range(PARTS):
        loads[2 * i].wait()
        loads[2 * i + 1].wait()
        parts = split2(z_ref[:, part(i)])
        z1_ref[:, part(i)], z2_ref[:, part(i)] = parts
        start = split2(s_ref[part(i), :])
        for upper in halves(z_ref.shape[0]):
            term = product3([p[upper] for p in parts], start, 1, 0)
            w_ref[upper, :] = term if i == 0 else w_ref[upper, :] + term
    image_rows(other)
    pl.semaphore_wait(barrier, len(greet))
    pair = remote(x_ref.at[half_rows(other), :], pair_ref, pair_s, pair_r, at(mq, other, mz))
    pair.start()
    image_rows(mc)
    pair.wait()
    x_ref[half_rows(mc), :] = x_ref[half_rows(mc), :] + pair_ref[...]

    for i in range(PARTS):
        for j, (dx, dy) in enumerate(plane):
            q = plane_peer(dx, dy)
            remote(
                x_ref.at[slab_rows(mc, q), part(i)], plane_ref.at[i, j], plane_s.at[i], plane_r.at[i], at(q, mc, mz)
            ).start()

    def plane_all(i, send, recv):
        return remote(plane_ref.at[i], plane_ref.at[i], send.at[i], recv.at[i], at(mq, other, mz))

    def line_all(i):
        most = line_ref.at[i, pl.ds(0, nz - 1)]
        return remote(most, most, line_s.at[i], line_r.at[i], at(mq, other, mz))

    m1_ref[...] = contract(s_ref[...], s_ref[...], 0, 0)
    start_factor = (m1_ref, left1_ref, right1_ref)
    steps = steps_of(start_factor)
    cut1, cut2 = steps * CUT1 // 16, steps * CUT2 // 16
    factor_steps(start_factor, 0, cut1)
    for i in range(PARTS):
        plane_all(i, plane_s, plane_r).wait_recv()
        total = x_ref[slab_rows(mc, mq), part(i)]
        for j in range(len(plane)):
            total = total + plane_ref[i, j]
        line_ref[i, mz] = total
        own = line_ref.at[i, mz]
        for dz in line:
            remote(own, own, line_s.at[i], line_r.at[i], at(mq, mc, (mz + dz) % nz)).start()
    factor_steps(start_factor, cut1, cut2)
    for i in range(PARTS):
        line_all(i).wait_recv()
        full_ref[slab_rows(mc, mq), part(i)] = functools.reduce(jnp.add, [line_ref[i, z] for z in range(nz)])
        slab = full_ref.at[slab_rows(mc, mq), part(i)]
        for dx, dy in plane:
            remote(slab, slab, back_s.at[i], back_r.at[i], at(plane_peer(dx, dy), mc, mz)).start()
    factor_steps(start_factor, cut2, steps)
    start_inverse = split2(m1_ref[...])
    energy_all = jnp.sum(z_ref[...] * z_ref[...])

    def forward(i):
        block = full_ref.at[half_rows(mc), part(i)]
        return remote(block, block, fw_s.at[i], fw_r.at[i], at(mq, other, mz))

    for i in range(PARTS + 1):
        if i < PARTS:
            plane_all(i, back_s, back_r).wait_recv()
            forward(i).start()
        if i > 0:
            forward(i - 1).wait_recv()
            part_ref[...] = product3(start_inverse, split2(full_ref[:, part(i - 1)]), 1, 0)
            square = contract(part_ref[...], part_ref[...], 1, 1)
            m2_ref[...] = square if i == 1 else m2_ref[...] + square
            term = product3((z1_ref[:, part(i - 1)], z2_ref[:, part(i - 1)]), split2(part_ref[...]), 1, 1)
            w_ref[...] = term if i == 1 else w_ref[...] + term

    image_factor = (m2_ref, left2_ref, right2_ref)
    factor_steps(image_factor, 0, steps_of(image_factor))
    compressed = product3(split2(w_ref[...]), split2(m2_ref[...]), 1, 1)
    c_ref[...] = compressed
    energy_kept = jnp.sum(compressed * compressed)

    lane = lax.broadcasted_iota(jnp.int32, (1, 128), 1)
    e_ref[...] = jnp.where(lane == 0, energy_kept, jnp.where(lane == 1, energy_all, 0.0))
    ep_ref[mq] = e_ref[...]
    first = []
    for j, (dx, dy) in enumerate(plane):
        first.append(remote(e_ref, ep_ref.at[mq], ep_s.at[j], ep_r.at[j], at(plane_peer(dx, dy), mc, mz)))
        first[-1].start()
    for copy in first:
        copy.wait()
    e_ref[...] = functools.reduce(jnp.add, [ep_ref[q] for q in range(nq)])
    spot = mz * 2 + mc
    eq_ref[spot] = e_ref[...]
    second = []
    for j, (dz, dc) in enumerate([(dz, dc) for dc in range(2) for dz in [*line, 0] if dz or dc]):
        second.append(
            remote(e_ref, eq_ref.at[spot], eq_s.at[j], eq_r.at[j], at(mq, (mc + dc) % 2, (mz + dz) % nz))
        )
        second[-1].start()
    for i in range(PARTS):
        plane_all(i, plane_s, plane_r).wait_send()
        line_all(i).wait_send()
        plane_all(i, back_s, back_r).wait_send()
        forward(i).wait_send()
    for copy in second:
        copy.wait()
    sums = functools.reduce(jnp.add, [eq_ref[i] for i in range(2 * nz)])
    tail_ref[...] = 1.0 - sums[:, 0:1] / sums[:, 1:2]


def local(sizes, factor, start_block):
    nx, ny, nz = sizes
    nq = nx * ny
    depth, rank = start_block.shape
    half = rank // 2
    rows, cols = half // nq, depth // PARTS
    vmem = pl.BlockSpec(memory_space=pltpu.VMEM)
    hbm = pl.BlockSpec(memory_space=pltpu.HBM)
    dma = pltpu.SemaphoreType.DMA
    compressed, tail = pl.pallas_call(
        functools.partial(kernel, sizes),
        out_shape=(
            jax.ShapeDtypeStruct((factor.shape[0], rank), F32),
            jax.ShapeDtypeStruct((1, 1), F32),
        ),
        in_specs=[hbm, hbm],
        out_specs=(vmem, vmem),
        scratch_shapes=[
            pltpu.VMEM(factor.shape, F32),
            pltpu.VMEM(start_block.shape, F32),
            pltpu.VMEM((factor.shape[0], rank), F32),
            pltpu.VMEM((rank, depth), F32),
            pltpu.VMEM((half, depth), F32),
            pltpu.VMEM((PARTS, nq - 1, rows, cols), F32),
            pltpu.VMEM((PARTS, nz, rows, cols), F32),
            pltpu.VMEM((rank, depth), F32),
            pltpu.VMEM((rank, cols), F32),
            pltpu.VMEM(factor.shape, jnp.bfloat16),
            pltpu.VMEM(factor.shape, jnp.bfloat16),
            pltpu.VMEM((rank, rank), F32),
            pltpu.VMEM((rank, 6 * PANEL1), jnp.bfloat16),
            pltpu.VMEM((6 * PANEL1, rank), jnp.bfloat16),
            pltpu.VMEM((rank, rank), F32),
            pltpu.VMEM((rank, 6 * PANEL2), jnp.bfloat16),
            pltpu.VMEM((6 * PANEL2, rank), jnp.bfloat16),
            pltpu.VMEM((1, 128), F32),
            pltpu.VMEM((nq, 1, 128), F32),
            pltpu.VMEM((2 * nz, 1, 128), F32),
            dma((PARTS,)),
            dma((PARTS,)),
            dma,
            dma,
            *[dma((PARTS,)) for _ in range(8)],
            dma((nq - 1,)),
            dma((nq - 1,)),
            dma((2 * nz - 1,)),
            dma((2 * nz - 1,)),
        ],
        compiler_params=pltpu.CompilerParams(
            collective_id=0, has_side_effects=True, vmem_limit_bytes=VMEM_GRANT
        ),
    )(factor, start_block)
    return compressed, tail[0, 0]


def solution(mesh):
    side = math.isqrt(mesh.shape["rows"] // 2)
    sizes = (side, side, mesh.shape["grp"])
    return jax.shard_map(
        functools.partial(local, sizes),
        mesh=mesh,
        in_specs=(P(AXES, None), P()),
        out_specs=(P(AXES, None), P()),
        check_vma=False,
    )
```

```python
import functools
import math

import jax
import jax.numpy as jnp
from jax import lax
from jax.experimental import pallas as pl
from jax.experimental.pallas import tpu as pltpu
from jax.sharding import PartitionSpec as P

AXES = ("rows", "grp")
HI = lax.Precision.HIGHEST
B = 16
PANEL1, PANEL2 = 64, 64
F32 = jnp.float32
PARTS = 4
VMEM_GRANT = 56_000_000
CUT1, CUT2 = 8, 12


def contract(a, b, da, db):
    return lax.dot_general(a, b, (((da,), (db,)), ((), ())), precision=HI, preferred_element_type=F32)


def split2(x):
    a = x.astype(jnp.bfloat16)
    return a, (x - a.astype(F32)).astype(jnp.bfloat16)


def product3(a, b, da, db):
    def term(x, y):
        return lax.dot_general(x, y, (((da,), (db,)), ((), ())), preferred_element_type=F32)

    return term(a[0], b[0]) + (term(a[0], b[1]) + term(a[1], b[0]))


def split3(x):
    a = x.astype(jnp.bfloat16).astype(F32)
    rest = x - a
    b = rest.astype(jnp.bfloat16).astype(F32)
    return a, b, (rest - b).astype(jnp.bfloat16).astype(F32)


def factor_step(m_ref, left_ref, right_ref, k):
    n = m_ref.shape[1]
    panel_rows = right_ref.shape[0] // 6
    row0 = pl.multiple_of(k * panel_rows, panel_rows)
    groups = panel_rows // 8
    rows8 = lax.broadcasted_iota(jnp.int32, (8, 128), 0)
    left, right = left_ref[...], right_ref[...]
    own = jnp.dot(left_ref[pl.ds(row0, panel_rows), :], right, preferred_element_type=F32)
    lanes = lax.broadcasted_iota(jnp.int32, (panel_rows, n), 1) - row0
    panel = jnp.where((lanes >= -panel_rows) & (lanes < 0), 0.0, m_ref[pl.ds(row0, panel_rows), :]) - own
    cols = lax.broadcasted_iota(jnp.int32, (n, n), 1) - row0
    update = jnp.dot(left, right, preferred_element_type=F32)
    below = lax.broadcasted_iota(jnp.int32, (n, n), 0) >= row0
    m_ref[...] = jnp.where(below & (cols >= -panel_rows) & (cols < 0), 0.0, m_ref[...]) - update
    wide = [panel[8 * g : 8 * g + 8] for g in range(groups)]
    pivots = [jnp.ones((8, 128), F32) for _ in range(groups)]
    lane8 = lanes[:8]
    place8 = lax.broadcasted_iota(jnp.int32, (8, n), 0)
    upper = row0 >= 128
    for b in range(panel_rows // B):
        first = b * B // 8
        lane0 = row0 % 128 + b * B
        column = {}
        for c in range(B):
            idx = jnp.full((8, 128), lane0 + c, jnp.int32)
            for g in range(first + c // 8, groups):
                column[c, g] = jnp.take_along_axis(jnp.where(upper, wide[g][:, 128:], wide[g][:, :128]), idx, axis=1)
        in_block = (lane8 >= b * B) & (lane8 < b * B + B)
        for g in range(first, groups):
            unit = jnp.where(lane8 == 8 * g + place8, 1.0, 0.0) if g < first + B // 8 else 0.0
            wide[g] = jnp.where(in_block, unit, wide[g])
        for c in range(B):
            gc, rc = first + c // 8, c % 8
            pivot = jnp.broadcast_to(column[c, gc][rc : rc + 1, :], (8, 128))
            pivots[gc] = jnp.where(rows8 == rc, pivot, pivots[gc])
            scale = 1.0 / pivot
            mult = {g: column[c, g] * scale for g in range(gc, groups)}
            mult[gc] = jnp.where(rows8 > rc, mult[gc], 0.0)
            pivot_row = jnp.broadcast_to(wide[gc][rc : rc + 1, :], (8, n))
            for d in range(c + 1, B):
                gd, rd = first + d // 8, d % 8
                entry = jnp.broadcast_to(column[c, gd][rd : rd + 1, :], (8, 128))
                for g in range(gd, groups):
                    column[d, g] = column[d, g] - mult[g] * entry
            for g in range(gc, groups):
                wide[g] = wide[g] - jnp.tile(mult[g], (1, n // 128)) * pivot_row
    final = []
    for g in range(groups):
        s = lax.rsqrt(pivots[g])
        s = s * (1.5 - 0.5 * pivots[g] * s * s)
        final.append(wide[g] * jnp.tile(s, (1, n // 128)))
    u = jnp.concatenate(final, axis=0)
    inside = lax.broadcasted_iota(jnp.int32, (panel_rows, n), 0)
    u = jnp.where((lanes < panel_rows) & (lanes > inside), 0.0, u)
    a, b, c = split3(u)
    right_ref[...] = jnp.concatenate([a, b, a, c, b, a], axis=0).astype(jnp.bfloat16)
    a, b, c = (jnp.where(lanes >= panel_rows, t, 0.0) for t in (a, b, c))
    left_ref[...] = jnp.concatenate([a, a, b, a, b, c], axis=0).T.astype(jnp.bfloat16)
    m_ref[pl.ds(row0, panel_rows), :] = u


def factor_steps(refs, lo, hi):
    m_ref, left_ref, right_ref = refs
    n = m_ref.shape[1]
    if lo == 0:
        left_ref[...] = jnp.zeros_like(left_ref)
        right_ref[...] = jnp.zeros_like(right_ref)

    def body(k, carry):
        factor_step(m_ref, left_ref, right_ref, k)
        return carry

    lax.fori_loop(lo, hi, body, 0)
    if hi == steps_of(refs):
        rows, cols = (lax.broadcasted_iota(jnp.int32, (n, n), d) for d in range(2))
        m_ref[...] = jnp.where(rows >= cols, m_ref[...], 0.0)


def steps_of(refs):
    return refs[0].shape[0] * 6 // refs[2].shape[0]


def kernel(
    sizes,
    z_hbm,
    s_hbm,
    c_ref,
    tail_ref,
    z_ref,
    s_ref,
    w_ref,
    x_ref,
    pair_ref,
    plane_ref,
    line_ref,
    full_ref,
    part_ref,
    z1_ref,
    z2_ref,
    m1_ref,
    left1_ref,
    right1_ref,
    m2_ref,
    left2_ref,
    right2_ref,
    e_ref,
    ep_ref,
    eq_ref,
    *sems,
):
    nx, ny, nz = sizes
    (z_in, s_in, pair_s, pair_r, plane_s, plane_r, line_s, line_r, back_s, back_r, fw_s, fw_r, ep_s, ep_r, eq_s, eq_r) = sems
    nq = nx * ny
    rank, depth = s_ref.shape[1], s_ref.shape[0]
    half = rank // 2
    rows, cols = half // nq, depth // PARTS
    me = lax.axis_index("rows")
    mz = lax.axis_index("grp")
    mc = me % 2
    mq = me // 2
    mx, my = mq // ny, mq % ny

    def at(q, c, z):
        return {"rows": q * 2 + c, "grp": z}

    def plane_peer(dx, dy):
        return ((mx + dx) % nx) * ny + (my + dy) % ny

    far = lambda d, n: min(d, n - d)
    plane = [(dx, dy) for dx in range(nx) for dy in range(ny) if dx or dy]
    plane.sort(key=lambda d: (-far(d[0], nx) - far(d[1], ny), d))
    line = sorted(range(1, nz), key=lambda d: (-far(d, nz), d))
    other = 1 - mc

    def part(i):
        return pl.ds(i * cols, cols)

    loads = []
    for i in range(PARTS):
        loads.append(pltpu.make_async_copy(z_hbm.at[:, part(i)], z_ref.at[:, part(i)], z_in.at[i]))
        loads.append(pltpu.make_async_copy(s_hbm.at[part(i), :], s_ref.at[part(i), :], s_in.at[i]))
    for copy in loads:
        copy.start()

    barrier = pltpu.get_barrier_semaphore()
    greet = [at(mq, other, mz)]
    greet += [at(plane_peer(dx, dy), mc, mz) for dx, dy in plane]
    greet += [at(mq, mc, (mz + dz) % nz) for dz in line]
    greet += [at(mq, other, (mz + dz) % nz) for dz in line]
    for device in greet:
        pl.semaphore_signal(barrier, inc=1, device_id=device, device_id_type=pl.DeviceIdType.MESH)

    def remote(src, dst, send, recv, device):
        return pltpu.make_async_remote_copy(
            src_ref=src, dst_ref=dst, send_sem=send, recv_sem=recv, device_id=device, device_id_type=pl.DeviceIdType.MESH
        )

    def half_rows(c):
        return pl.ds(pl.multiple_of(c * half, half), half)

    def slab_rows(c, q):
        return pl.ds(pl.multiple_of(c * half + q * rows, rows), rows)

    def halves(n):
        return slice(0, n // 2), slice(n // 2, n)

    def image_rows(c):
        rows_of_c = split2(w_ref[:, half_rows(c)].T)
        for h in halves(depth):
            x_ref[half_rows(c), h] = product3(rows_of_c, (z1_ref[:, h], z2_ref[:, h]), 1, 0)

    for i in range(PARTS):
        loads[2 * i].wait()
        loads[2 * i + 1].wait()
        parts = split2(z_ref[:, part(i)])
        z1_ref[:, part(i)], z2_ref[:, part(i)] = parts
        start = split2(s_ref[part(i), :])
        for upper in halves(z_ref.shape[0]):
            term = product3([p[upper] for p in parts], start, 1, 0)
            w_ref[upper, :] = term if i == 0 else w_ref[upper, :] + term
    image_rows(other)
    pl.semaphore_wait(barrier, len(greet))
    pair = remote(x_ref.at[half_rows(other), :], pair_ref, pair_s, pair_r, at(mq, other, mz))
    pair.start()
    image_rows(mc)
    for h in halves(rank):
        m1_ref[h, :] = contract(s_ref[:, h], s_ref[...], 0, 0)
    pair.wait()
    x_ref[half_rows(mc), :] = x_ref[half_rows(mc), :] + pair_ref[...]

    for i in range(PARTS):
        for j, (dx, dy) in enumerate(plane):
            q = plane_peer(dx, dy)
            remote(
                x_ref.at[slab_rows(mc, q), part(i)], plane_ref.at[i, j], plane_s.at[i], plane_r.at[i], at(q, mc, mz)
            ).start()

    def plane_all(i, send, recv):
        return remote(plane_ref.at[i], plane_ref.at[i], send.at[i], recv.at[i], at(mq, other, mz))

    def line_all(i):
        most = line_ref.at[i, pl.ds(0, nz - 1)]
        return remote(most, most, line_s.at[i], line_r.at[i], at(mq, other, mz))

    start_factor = (m1_ref, left1_ref, right1_ref)
    steps = steps_of(start_factor)
    cut1, cut2 = steps * CUT1 // 16, steps * CUT2 // 16
    factor_steps(start_factor, 0, cut1)
    for i in range(PARTS):
        plane_all(i, plane_s, plane_r).wait_recv()
        total = x_ref[slab_rows(mc, mq), part(i)]
        for j in range(len(plane)):
            total = total + plane_ref[i, j]
        line_ref[i, mz] = total
        own = line_ref.at[i, mz]
        for dz in line:
            remote(own, own, line_s.at[i], line_r.at[i], at(mq, mc, (mz + dz) % nz)).start()
    factor_steps(start_factor, cut1, cut2)
    for i in range(PARTS):
        line_all(i).wait_recv()
        full_ref[slab_rows(mc, mq), part(i)] = functools.reduce(jnp.add, [line_ref[i, z] for z in range(nz)])
        slab = full_ref.at[slab_rows(mc, mq), part(i)]
        for dx, dy in plane:
            remote(slab, slab, back_s.at[i], back_r.at[i], at(plane_peer(dx, dy), mc, mz)).start()
    factor_steps(start_factor, cut2, steps)
    start_inverse = split2(m1_ref[...])
    energy_all = jnp.sum(z_ref[...] * z_ref[...])

    def forward(i):
        block = full_ref.at[half_rows(mc), part(i)]
        return remote(block, block, fw_s.at[i], fw_r.at[i], at(mq, other, mz))

    for i in range(PARTS + 1):
        if i < PARTS:
            plane_all(i, back_s, back_r).wait_recv()
            forward(i).start()
        if i > 0:
            forward(i - 1).wait_recv()
            part_ref[...] = product3(start_inverse, split2(full_ref[:, part(i - 1)]), 1, 0)
            square = contract(part_ref[...], part_ref[...], 1, 1)
            m2_ref[...] = square if i == 1 else m2_ref[...] + square
            term = product3((z1_ref[:, part(i - 1)], z2_ref[:, part(i - 1)]), split2(part_ref[...]), 1, 1)
            w_ref[...] = term if i == 1 else w_ref[...] + term

    image_factor = (m2_ref, left2_ref, right2_ref)
    factor_steps(image_factor, 0, steps_of(image_factor))
    compressed = product3(split2(w_ref[...]), split2(m2_ref[...]), 1, 1)
    c_ref[...] = compressed
    energy_kept = jnp.sum(compressed * compressed)

    lane = lax.broadcasted_iota(jnp.int32, (1, 128), 1)
    e_ref[...] = jnp.where(lane == 0, energy_kept, jnp.where(lane == 1, energy_all, 0.0))
    ep_ref[mq] = e_ref[...]
    first = []
    for j, (dx, dy) in enumerate(plane):
        first.append(remote(e_ref, ep_ref.at[mq], ep_s.at[j], ep_r.at[j], at(plane_peer(dx, dy), mc, mz)))
        first[-1].start()
    for copy in first:
        copy.wait()
    e_ref[...] = functools.reduce(jnp.add, [ep_ref[q] for q in range(nq)])
    spot = mz * 2 + mc
    eq_ref[spot] = e_ref[...]
    second = []
    for j, (dz, dc) in enumerate([(dz, dc) for dc in range(2) for dz in [*line, 0] if dz or dc]):
        second.append(
            remote(e_ref, eq_ref.at[spot], eq_s.at[j], eq_r.at[j], at(mq, (mc + dc) % 2, (mz + dz) % nz))
        )
        second[-1].start()
    for i in range(PARTS):
        plane_all(i, plane_s, plane_r).wait_send()
        line_all(i).wait_send()
        plane_all(i, back_s, back_r).wait_send()
        forward(i).wait_send()
    for copy in second:
        copy.wait()
    sums = functools.reduce(jnp.add, [eq_ref[i] for i in range(2 * nz)])
    tail_ref[...] = 1.0 - sums[:, 0:1] / sums[:, 1:2]


def local(sizes, factor, start_block):
    nx, ny, nz = sizes
    nq = nx * ny
    depth, rank = start_block.shape
    half = rank // 2
    rows, cols = half // nq, depth // PARTS
    vmem = pl.BlockSpec(memory_space=pltpu.VMEM)
    hbm = pl.BlockSpec(memory_space=pltpu.HBM)
    dma = pltpu.SemaphoreType.DMA
    compressed, tail = pl.pallas_call(
        functools.partial(kernel, sizes),
        out_shape=(
            jax.ShapeDtypeStruct((factor.shape[0], rank), F32),
            jax.ShapeDtypeStruct((1, 1), F32),
        ),
        in_specs=[hbm, hbm],
        out_specs=(vmem, vmem),
        scratch_shapes=[
            pltpu.VMEM(factor.shape, F32),
            pltpu.VMEM(start_block.shape, F32),
            pltpu.VMEM((factor.shape[0], rank), F32),
            pltpu.VMEM((rank, depth), F32),
            pltpu.VMEM((half, depth), F32),
            pltpu.VMEM((PARTS, nq - 1, rows, cols), F32),
            pltpu.VMEM((PARTS, nz, rows, cols), F32),
            pltpu.VMEM((rank, depth), F32),
            pltpu.VMEM((rank, cols), F32),
            pltpu.VMEM(factor.shape, jnp.bfloat16),
            pltpu.VMEM(factor.shape, jnp.bfloat16),
            pltpu.VMEM((rank, rank), F32),
            pltpu.VMEM((rank, 6 * PANEL1), jnp.bfloat16),
            pltpu.VMEM((6 * PANEL1, rank), jnp.bfloat16),
            pltpu.VMEM((rank, rank), F32),
            pltpu.VMEM((rank, 6 * PANEL2), jnp.bfloat16),
            pltpu.VMEM((6 * PANEL2, rank), jnp.bfloat16),
            pltpu.VMEM((1, 128), F32),
            pltpu.VMEM((nq, 1, 128), F32),
            pltpu.VMEM((2 * nz, 1, 128), F32),
            dma((PARTS,)),
            dma((PARTS,)),
            dma,
            dma,
            *[dma((PARTS,)) for _ in range(8)],
            dma((nq - 1,)),
            dma((nq - 1,)),
            dma((2 * nz - 1,)),
            dma((2 * nz - 1,)),
        ],
        compiler_params=pltpu.CompilerParams(
            collective_id=0, has_side_effects=True, vmem_limit_bytes=VMEM_GRANT
        ),
    )(factor, start_block)
    return compressed, tail[0, 0]


def solution(mesh):
    side = math.isqrt(mesh.shape["rows"] // 2)
    sizes = (side, side, mesh.shape["grp"])
    return jax.shard_map(
        functools.partial(local, sizes),
        mesh=mesh,
        in_specs=(P(AXES, None), P()),
        out_specs=(P(AXES, None), P()),
        check_vma=False,
    )
```

```python
import functools
import math

import jax
import jax.numpy as jnp
from jax import lax
from jax.experimental import pallas as pl
from jax.experimental.pallas import tpu as pltpu
from jax.sharding import PartitionSpec as P

AXES = ("rows", "grp")
HI = lax.Precision.HIGHEST
B = 16
PANEL1, PANEL2 = 64, 64
F32 = jnp.float32
LOADS = 4
WIDTHS = (1, 2, 2, 2, 1)
PARTS = len(WIDTHS)
VMEM_GRANT = 56_000_000
CUT1, CUT2 = 8, 12


def contract(a, b, da, db):
    return lax.dot_general(a, b, (((da,), (db,)), ((), ())), precision=HI, preferred_element_type=F32)


def split2(x):
    a = x.astype(jnp.bfloat16)
    return a, (x - a.astype(F32)).astype(jnp.bfloat16)


def product3(a, b, da, db):
    def term(x, y):
        return lax.dot_general(x, y, (((da,), (db,)), ((), ())), preferred_element_type=F32)

    return term(a[0], b[0]) + (term(a[0], b[1]) + term(a[1], b[0]))


def split3(x):
    a = x.astype(jnp.bfloat16).astype(F32)
    rest = x - a
    b = rest.astype(jnp.bfloat16).astype(F32)
    return a, b, (rest - b).astype(jnp.bfloat16).astype(F32)


def factor_step(m_ref, left_ref, right_ref, k):
    n = m_ref.shape[1]
    panel_rows = right_ref.shape[0] // 6
    row0 = pl.multiple_of(k * panel_rows, panel_rows)
    groups = panel_rows // 8
    rows8 = lax.broadcasted_iota(jnp.int32, (8, 128), 0)
    left, right = left_ref[...], right_ref[...]
    own = jnp.dot(left_ref[pl.ds(row0, panel_rows), :], right, preferred_element_type=F32)
    lanes = lax.broadcasted_iota(jnp.int32, (panel_rows, n), 1) - row0
    panel = jnp.where((lanes >= -panel_rows) & (lanes < 0), 0.0, m_ref[pl.ds(row0, panel_rows), :]) - own
    cols = lax.broadcasted_iota(jnp.int32, (n, n), 1) - row0
    update = jnp.dot(left, right, preferred_element_type=F32)
    below = lax.broadcasted_iota(jnp.int32, (n, n), 0) >= row0
    m_ref[...] = jnp.where(below & (cols >= -panel_rows) & (cols < 0), 0.0, m_ref[...]) - update
    wide = [panel[8 * g : 8 * g + 8] for g in range(groups)]
    pivots = [jnp.ones((8, 128), F32) for _ in range(groups)]
    lane8 = lanes[:8]
    place8 = lax.broadcasted_iota(jnp.int32, (8, n), 0)
    upper = row0 >= 128
    for b in range(panel_rows // B):
        first = b * B // 8
        lane0 = row0 % 128 + b * B
        column = {}
        for c in range(B):
            idx = jnp.full((8, 128), lane0 + c, jnp.int32)
            for g in range(first + c // 8, groups):
                column[c, g] = jnp.take_along_axis(jnp.where(upper, wide[g][:, 128:], wide[g][:, :128]), idx, axis=1)
        in_block = (lane8 >= b * B) & (lane8 < b * B + B)
        for g in range(first, groups):
            unit = jnp.where(lane8 == 8 * g + place8, 1.0, 0.0) if g < first + B // 8 else 0.0
            wide[g] = jnp.where(in_block, unit, wide[g])
        for c in range(B):
            gc, rc = first + c // 8, c % 8
            pivot = jnp.broadcast_to(column[c, gc][rc : rc + 1, :], (8, 128))
            pivots[gc] = jnp.where(rows8 == rc, pivot, pivots[gc])
            scale = 1.0 / pivot
            mult = {g: column[c, g] * scale for g in range(gc, groups)}
            mult[gc] = jnp.where(rows8 > rc, mult[gc], 0.0)
            pivot_row = jnp.broadcast_to(wide[gc][rc : rc + 1, :], (8, n))
            for d in range(c + 1, B):
                gd, rd = first + d // 8, d % 8
                entry = jnp.broadcast_to(column[c, gd][rd : rd + 1, :], (8, 128))
                for g in range(gd, groups):
                    column[d, g] = column[d, g] - mult[g] * entry
            for g in range(gc, groups):
                wide[g] = wide[g] - jnp.tile(mult[g], (1, n // 128)) * pivot_row
    final = []
    for g in range(groups):
        s = lax.rsqrt(pivots[g])
        s = s * (1.5 - 0.5 * pivots[g] * s * s)
        final.append(wide[g] * jnp.tile(s, (1, n // 128)))
    u = jnp.concatenate(final, axis=0)
    inside = lax.broadcasted_iota(jnp.int32, (panel_rows, n), 0)
    u = jnp.where((lanes < panel_rows) & (lanes > inside), 0.0, u)
    a, b, c = split3(u)
    right_ref[...] = jnp.concatenate([a, b, a, c, b, a], axis=0).astype(jnp.bfloat16)
    a, b, c = (jnp.where(lanes >= panel_rows, t, 0.0) for t in (a, b, c))
    left_ref[...] = jnp.concatenate([a, a, b, a, b, c], axis=0).T.astype(jnp.bfloat16)
    m_ref[pl.ds(row0, panel_rows), :] = u


def factor_steps(refs, lo, hi):
    m_ref, left_ref, right_ref = refs
    n = m_ref.shape[1]
    if lo == 0:
        left_ref[...] = jnp.zeros_like(left_ref)
        right_ref[...] = jnp.zeros_like(right_ref)

    def body(k, carry):
        factor_step(m_ref, left_ref, right_ref, k)
        return carry

    lax.fori_loop(lo, hi, body, 0)
    if hi == steps_of(refs):
        rows, cols = (lax.broadcasted_iota(jnp.int32, (n, n), d) for d in range(2))
        m_ref[...] = jnp.where(rows >= cols, m_ref[...], 0.0)


def steps_of(refs):
    return refs[0].shape[0] * 6 // refs[2].shape[0]


def kernel(
    sizes,
    z_hbm,
    s_hbm,
    c_ref,
    tail_ref,
    z_ref,
    s_ref,
    w_ref,
    x_ref,
    pair_ref,
    plane_ref,
    line_ref,
    full_ref,
    part_ref,
    z1_ref,
    z2_ref,
    m1_ref,
    left1_ref,
    right1_ref,
    m2_ref,
    left2_ref,
    right2_ref,
    e_ref,
    ep_ref,
    eq_ref,
    *sems,
):
    nx, ny, nz = sizes
    (z_in, s_in, pair_s, pair_r, plane_s, plane_r, line_s, line_r, back_s, back_r, fw_s, fw_r, ep_s, ep_r, eq_s, eq_r) = sems
    nq = nx * ny
    rank, depth = s_ref.shape[1], s_ref.shape[0]
    half = rank // 2
    rows, unit = half // nq, depth // sum(WIDTHS)
    me = lax.axis_index("rows")
    mz = lax.axis_index("grp")
    mc = me % 2
    mq = me // 2
    mx, my = mq // ny, mq % ny

    def at(q, c, z):
        return {"rows": q * 2 + c, "grp": z}

    def plane_peer(dx, dy):
        return ((mx + dx) % nx) * ny + (my + dy) % ny

    far = lambda d, n: min(d, n - d)
    plane = [(dx, dy) for dx in range(nx) for dy in range(ny) if dx or dy]
    plane.sort(key=lambda d: (-far(d[0], nx) - far(d[1], ny), d))
    line = sorted(range(1, nz), key=lambda d: (-far(d, nz), d))
    other = 1 - mc

    def load_part(i):
        return slice(i * (depth // LOADS), (i + 1) * (depth // LOADS))

    def part(i):
        return slice(sum(WIDTHS[:i]) * unit, sum(WIDTHS[: i + 1]) * unit)

    def width(i):
        return slice(0, WIDTHS[i] * unit)

    loads = []
    for i in range(LOADS):
        loads.append(pltpu.make_async_copy(z_hbm.at[:, load_part(i)], z_ref.at[:, load_part(i)], z_in.at[i]))
        loads.append(pltpu.make_async_copy(s_hbm.at[load_part(i), :], s_ref.at[load_part(i), :], s_in.at[i]))
    for copy in loads:
        copy.start()

    barrier = pltpu.get_barrier_semaphore()
    greet = [at(mq, other, mz)]
    greet += [at(plane_peer(dx, dy), mc, mz) for dx, dy in plane]
    greet += [at(mq, mc, (mz + dz) % nz) for dz in line]
    greet += [at(mq, other, (mz + dz) % nz) for dz in line]
    for device in greet:
        pl.semaphore_signal(barrier, inc=1, device_id=device, device_id_type=pl.DeviceIdType.MESH)

    def remote(src, dst, send, recv, device):
        return pltpu.make_async_remote_copy(
            src_ref=src, dst_ref=dst, send_sem=send, recv_sem=recv, device_id=device, device_id_type=pl.DeviceIdType.MESH
        )

    def half_rows(c):
        return pl.ds(pl.multiple_of(c * half, half), half)

    def slab_rows(c, q):
        return pl.ds(pl.multiple_of(c * half + q * rows, rows), rows)

    def halves(n):
        return slice(0, n // 2), slice(n // 2, n)

    def image_rows(c):
        rows_of_c = split2(w_ref[:, half_rows(c)].T)
        for h in halves(depth):
            x_ref[half_rows(c), h] = product3(rows_of_c, (z1_ref[:, h], z2_ref[:, h]), 1, 0)

    for i in range(LOADS):
        loads[2 * i].wait()
        loads[2 * i + 1].wait()
        parts = split2(z_ref[:, load_part(i)])
        z1_ref[:, load_part(i)], z2_ref[:, load_part(i)] = parts
        start = split2(s_ref[load_part(i), :])
        for upper in halves(z_ref.shape[0]):
            term = product3([p[upper] for p in parts], start, 1, 0)
            w_ref[upper, :] = term if i == 0 else w_ref[upper, :] + term
    image_rows(other)
    pl.semaphore_wait(barrier, len(greet))
    pair = remote(x_ref.at[half_rows(other), :], pair_ref, pair_s, pair_r, at(mq, other, mz))
    pair.start()
    image_rows(mc)
    for h in halves(rank):
        m1_ref[h, :] = contract(s_ref[:, h], s_ref[...], 0, 0)
    pair.wait()
    x_ref[half_rows(mc), :] = x_ref[half_rows(mc), :] + pair_ref[...]

    for i in range(PARTS):
        for j, (dx, dy) in enumerate(plane):
            q = plane_peer(dx, dy)
            remote(
                x_ref.at[slab_rows(mc, q), part(i)], plane_ref.at[i, j, :, width(i)], plane_s.at[i], plane_r.at[i], at(q, mc, mz)
            ).start()

    def plane_all(i, send, recv):
        every = plane_ref.at[i, :, :, width(i)]
        return remote(every, every, send.at[i], recv.at[i], at(mq, other, mz))

    def line_all(i):
        most = line_ref.at[i, pl.ds(0, nz - 1), :, width(i)]
        return remote(most, most, line_s.at[i], line_r.at[i], at(mq, other, mz))

    start_factor = (m1_ref, left1_ref, right1_ref)
    steps = steps_of(start_factor)
    cut1, cut2 = steps * CUT1 // 16, steps * CUT2 // 16
    factor_steps(start_factor, 0, cut1)
    for i in range(PARTS):
        plane_all(i, plane_s, plane_r).wait_recv()
        total = x_ref[slab_rows(mc, mq), part(i)]
        for j in range(len(plane)):
            total = total + plane_ref[i, j, :, width(i)]
        line_ref[i, mz, :, width(i)] = total
        own = line_ref.at[i, mz, :, width(i)]
        for dz in line:
            remote(own, own, line_s.at[i], line_r.at[i], at(mq, mc, (mz + dz) % nz)).start()
    factor_steps(start_factor, cut1, cut2)
    for i in range(PARTS):
        line_all(i).wait_recv()
        full_ref[slab_rows(mc, mq), part(i)] = functools.reduce(jnp.add, [line_ref[i, z, :, width(i)] for z in range(nz)])
        slab = full_ref.at[slab_rows(mc, mq), part(i)]
        for dx, dy in plane:
            remote(slab, slab, back_s.at[i], back_r.at[i], at(plane_peer(dx, dy), mc, mz)).start()
    factor_steps(start_factor, cut2, steps)
    start_inverse = split2(m1_ref[...])
    energy_all = jnp.sum(z_ref[...] * z_ref[...])

    def forward(i):
        block = full_ref.at[half_rows(mc), part(i)]
        return remote(block, block, fw_s.at[i], fw_r.at[i], at(mq, other, mz))

    for i in range(PARTS + 1):
        if i < PARTS:
            plane_all(i, back_s, back_r).wait_recv()
            forward(i).start()
        if i > 0:
            forward(i - 1).wait_recv()
            image = part_ref.at[:, width(i - 1)]
            image[...] = product3(start_inverse, split2(full_ref[:, part(i - 1)]), 1, 0)
            square = contract(image[...], image[...], 1, 1)
            m2_ref[...] = square if i == 1 else m2_ref[...] + square
            term = product3((z1_ref[:, part(i - 1)], z2_ref[:, part(i - 1)]), split2(image[...]), 1, 1)
            w_ref[...] = term if i == 1 else w_ref[...] + term

    image_factor = (m2_ref, left2_ref, right2_ref)
    factor_steps(image_factor, 0, steps_of(image_factor))
    compressed = product3(split2(w_ref[...]), split2(m2_ref[...]), 1, 1)
    c_ref[...] = compressed
    energy_kept = jnp.sum(compressed * compressed)

    lane = lax.broadcasted_iota(jnp.int32, (1, 128), 1)
    e_ref[...] = jnp.where(lane == 0, energy_kept, jnp.where(lane == 1, energy_all, 0.0))
    ep_ref[mq] = e_ref[...]
    first = []
    for j, (dx, dy) in enumerate(plane):
        first.append(remote(e_ref, ep_ref.at[mq], ep_s.at[j], ep_r.at[j], at(plane_peer(dx, dy), mc, mz)))
        first[-1].start()
    for copy in first:
        copy.wait()
    e_ref[...] = functools.reduce(jnp.add, [ep_ref[q] for q in range(nq)])
    spot = mz * 2 + mc
    eq_ref[spot] = e_ref[...]
    second = []
    for j, (dz, dc) in enumerate([(dz, dc) for dc in range(2) for dz in [*line, 0] if dz or dc]):
        second.append(
            remote(e_ref, eq_ref.at[spot], eq_s.at[j], eq_r.at[j], at(mq, (mc + dc) % 2, (mz + dz) % nz))
        )
        second[-1].start()
    for i in range(PARTS):
        plane_all(i, plane_s, plane_r).wait_send()
        line_all(i).wait_send()
        plane_all(i, back_s, back_r).wait_send()
        forward(i).wait_send()
    for copy in second:
        copy.wait()
    sums = functools.reduce(jnp.add, [eq_ref[i] for i in range(2 * nz)])
    tail_ref[...] = 1.0 - sums[:, 0:1] / sums[:, 1:2]


def local(sizes, factor, start_block):
    nx, ny, nz = sizes
    nq = nx * ny
    depth, rank = start_block.shape
    half = rank // 2
    rows, cols = half // nq, depth // sum(WIDTHS) * max(WIDTHS)
    vmem = pl.BlockSpec(memory_space=pltpu.VMEM)
    hbm = pl.BlockSpec(memory_space=pltpu.HBM)
    dma = pltpu.SemaphoreType.DMA
    compressed, tail = pl.pallas_call(
        functools.partial(kernel, sizes),
        out_shape=(
            jax.ShapeDtypeStruct((factor.shape[0], rank), F32),
            jax.ShapeDtypeStruct((1, 1), F32),
        ),
        in_specs=[hbm, hbm],
        out_specs=(vmem, vmem),
        scratch_shapes=[
            pltpu.VMEM(factor.shape, F32),
            pltpu.VMEM(start_block.shape, F32),
            pltpu.VMEM((factor.shape[0], rank), F32),
            pltpu.VMEM((rank, depth), F32),
            pltpu.VMEM((half, depth), F32),
            pltpu.VMEM((PARTS, nq - 1, rows, cols), F32),
            pltpu.VMEM((PARTS, nz, rows, cols), F32),
            pltpu.VMEM((rank, depth), F32),
            pltpu.VMEM((rank, cols), F32),
            pltpu.VMEM(factor.shape, jnp.bfloat16),
            pltpu.VMEM(factor.shape, jnp.bfloat16),
            pltpu.VMEM((rank, rank), F32),
            pltpu.VMEM((rank, 6 * PANEL1), jnp.bfloat16),
            pltpu.VMEM((6 * PANEL1, rank), jnp.bfloat16),
            pltpu.VMEM((rank, rank), F32),
            pltpu.VMEM((rank, 6 * PANEL2), jnp.bfloat16),
            pltpu.VMEM((6 * PANEL2, rank), jnp.bfloat16),
            pltpu.VMEM((1, 128), F32),
            pltpu.VMEM((nq, 1, 128), F32),
            pltpu.VMEM((2 * nz, 1, 128), F32),
            dma((LOADS,)),
            dma((LOADS,)),
            dma,
            dma,
            *[dma((PARTS,)) for _ in range(8)],
            dma((nq - 1,)),
            dma((nq - 1,)),
            dma((2 * nz - 1,)),
            dma((2 * nz - 1,)),
        ],
        compiler_params=pltpu.CompilerParams(
            collective_id=0, has_side_effects=True, vmem_limit_bytes=VMEM_GRANT
        ),
    )(factor, start_block)
    return compressed, tail[0, 0]


def solution(mesh):
    side = math.isqrt(mesh.shape["rows"] // 2)
    sizes = (side, side, mesh.shape["grp"])
    return jax.shard_map(
        functools.partial(local, sizes),
        mesh=mesh,
        in_specs=(P(AXES, None), P()),
        out_specs=(P(AXES, None), P()),
        check_vma=False,
    )
```

```python
import functools
import math

import jax
import jax.numpy as jnp
from jax import lax
from jax.experimental import pallas as pl
from jax.experimental.pallas import tpu as pltpu
from jax.sharding import PartitionSpec as P

AXES = ("rows", "grp")
HI = lax.Precision.HIGHEST
B = 16
PANEL1, PANEL2 = 64, 64
F32 = jnp.float32
LOADS = 4
WIDTHS = (3, 3, 2)
PARTS = len(WIDTHS)
VMEM_GRANT = 56_000_000
CUT1, CUT2 = 8, 12


def contract(a, b, da, db):
    return lax.dot_general(a, b, (((da,), (db,)), ((), ())), precision=HI, preferred_element_type=F32)


def split2(x):
    a = x.astype(jnp.bfloat16)
    return a, (x - a.astype(F32)).astype(jnp.bfloat16)


def product3(a, b, da, db):
    def term(x, y):
        return lax.dot_general(x, y, (((da,), (db,)), ((), ())), preferred_element_type=F32)

    return term(a[0], b[0]) + (term(a[0], b[1]) + term(a[1], b[0]))


def split3(x):
    a = x.astype(jnp.bfloat16).astype(F32)
    rest = x - a
    b = rest.astype(jnp.bfloat16).astype(F32)
    return a, b, (rest - b).astype(jnp.bfloat16).astype(F32)


def factor_step(m_ref, left_ref, right_ref, k):
    n = m_ref.shape[1]
    panel_rows = right_ref.shape[0] // 6
    row0 = pl.multiple_of(k * panel_rows, panel_rows)
    groups = panel_rows // 8
    rows8 = lax.broadcasted_iota(jnp.int32, (8, 128), 0)
    left, right = left_ref[...], right_ref[...]
    own = jnp.dot(left_ref[pl.ds(row0, panel_rows), :], right, preferred_element_type=F32)
    lanes = lax.broadcasted_iota(jnp.int32, (panel_rows, n), 1) - row0
    panel = jnp.where((lanes >= -panel_rows) & (lanes < 0), 0.0, m_ref[pl.ds(row0, panel_rows), :]) - own
    cols = lax.broadcasted_iota(jnp.int32, (n, n), 1) - row0
    update = jnp.dot(left, right, preferred_element_type=F32)
    below = lax.broadcasted_iota(jnp.int32, (n, n), 0) >= row0
    m_ref[...] = jnp.where(below & (cols >= -panel_rows) & (cols < 0), 0.0, m_ref[...]) - update
    wide = [panel[8 * g : 8 * g + 8] for g in range(groups)]
    pivots = [jnp.ones((8, 128), F32) for _ in range(groups)]
    lane8 = lanes[:8]
    place8 = lax.broadcasted_iota(jnp.int32, (8, n), 0)
    upper = row0 >= 128
    for b in range(panel_rows // B):
        first = b * B // 8
        lane0 = row0 % 128 + b * B
        column = {}
        for c in range(B):
            idx = jnp.full((8, 128), lane0 + c, jnp.int32)
            for g in range(first + c // 8, groups):
                column[c, g] = jnp.take_along_axis(jnp.where(upper, wide[g][:, 128:], wide[g][:, :128]), idx, axis=1)
        in_block = (lane8 >= b * B) & (lane8 < b * B + B)
        for g in range(first, groups):
            unit = jnp.where(lane8 == 8 * g + place8, 1.0, 0.0) if g < first + B // 8 else 0.0
            wide[g] = jnp.where(in_block, unit, wide[g])
        for c in range(B):
            gc, rc = first + c // 8, c % 8
            pivot = jnp.broadcast_to(column[c, gc][rc : rc + 1, :], (8, 128))
            pivots[gc] = jnp.where(rows8 == rc, pivot, pivots[gc])
            scale = 1.0 / pivot
            mult = {g: column[c, g] * scale for g in range(gc, groups)}
            mult[gc] = jnp.where(rows8 > rc, mult[gc], 0.0)
            pivot_row = jnp.broadcast_to(wide[gc][rc : rc + 1, :], (8, n))
            for d in range(c + 1, B):
                gd, rd = first + d // 8, d % 8
                entry = jnp.broadcast_to(column[c, gd][rd : rd + 1, :], (8, 128))
                for g in range(gd, groups):
                    column[d, g] = column[d, g] - mult[g] * entry
            for g in range(gc, groups):
                wide[g] = wide[g] - jnp.tile(mult[g], (1, n // 128)) * pivot_row
    final = []
    for g in range(groups):
        s = lax.rsqrt(pivots[g])
        s = s * (1.5 - 0.5 * pivots[g] * s * s)
        final.append(wide[g] * jnp.tile(s, (1, n // 128)))
    u = jnp.concatenate(final, axis=0)
    inside = lax.broadcasted_iota(jnp.int32, (panel_rows, n), 0)
    u = jnp.where((lanes < panel_rows) & (lanes > inside), 0.0, u)
    a, b, c = split3(u)
    right_ref[...] = jnp.concatenate([a, b, a, c, b, a], axis=0).astype(jnp.bfloat16)
    a, b, c = (jnp.where(lanes >= panel_rows, t, 0.0) for t in (a, b, c))
    left_ref[...] = jnp.concatenate([a, a, b, a, b, c], axis=0).T.astype(jnp.bfloat16)
    m_ref[pl.ds(row0, panel_rows), :] = u


def factor_steps(refs, lo, hi):
    m_ref, left_ref, right_ref = refs
    n = m_ref.shape[1]
    if lo == 0:
        left_ref[...] = jnp.zeros_like(left_ref)
        right_ref[...] = jnp.zeros_like(right_ref)

    def body(k, carry):
        factor_step(m_ref, left_ref, right_ref, k)
        return carry

    lax.fori_loop(lo, hi, body, 0)
    if hi == steps_of(refs):
        rows, cols = (lax.broadcasted_iota(jnp.int32, (n, n), d) for d in range(2))
        m_ref[...] = jnp.where(rows >= cols, m_ref[...], 0.0)


def steps_of(refs):
    return refs[0].shape[0] * 6 // refs[2].shape[0]


def kernel(
    sizes,
    z_hbm,
    s_hbm,
    c_ref,
    tail_ref,
    z_ref,
    s_ref,
    w_ref,
    x_ref,
    pair_ref,
    plane_ref,
    line_ref,
    full_ref,
    part_ref,
    z1_ref,
    z2_ref,
    m1_ref,
    left1_ref,
    right1_ref,
    m2_ref,
    left2_ref,
    right2_ref,
    e_ref,
    ep_ref,
    eq_ref,
    *sems,
):
    nx, ny, nz = sizes
    (z_in, s_in, pair_s, pair_r, plane_s, plane_r, line_s, line_r, back_s, back_r, fw_s, fw_r, ep_s, ep_r, eq_s, eq_r) = sems
    nq = nx * ny
    rank, depth = s_ref.shape[1], s_ref.shape[0]
    half = rank // 2
    rows, unit = half // nq, depth // sum(WIDTHS)
    me = lax.axis_index("rows")
    mz = lax.axis_index("grp")
    mc = me % 2
    mq = me // 2
    mx, my = mq // ny, mq % ny

    def at(q, c, z):
        return {"rows": q * 2 + c, "grp": z}

    def plane_peer(dx, dy):
        return ((mx + dx) % nx) * ny + (my + dy) % ny

    far = lambda d, n: min(d, n - d)
    plane = [(dx, dy) for dx in range(nx) for dy in range(ny) if dx or dy]
    plane.sort(key=lambda d: (-far(d[0], nx) - far(d[1], ny), d))
    line = sorted(range(1, nz), key=lambda d: (-far(d, nz), d))
    other = 1 - mc

    def load_part(i):
        return slice(i * (depth // LOADS), (i + 1) * (depth // LOADS))

    def part(i):
        return slice(sum(WIDTHS[:i]) * unit, sum(WIDTHS[: i + 1]) * unit)

    def width(i):
        return slice(0, WIDTHS[i] * unit)

    loads = []
    for i in range(LOADS):
        loads.append(pltpu.make_async_copy(z_hbm.at[:, load_part(i)], z_ref.at[:, load_part(i)], z_in.at[i]))
        loads.append(pltpu.make_async_copy(s_hbm.at[load_part(i), :], s_ref.at[load_part(i), :], s_in.at[i]))
    for copy in loads:
        copy.start()

    barrier = pltpu.get_barrier_semaphore()
    greet = [at(mq, other, mz)]
    greet += [at(plane_peer(dx, dy), mc, mz) for dx, dy in plane]
    greet += [at(mq, mc, (mz + dz) % nz) for dz in line]
    greet += [at(mq, other, (mz + dz) % nz) for dz in line]
    for device in greet:
        pl.semaphore_signal(barrier, inc=1, device_id=device, device_id_type=pl.DeviceIdType.MESH)

    def remote(src, dst, send, recv, device):
        return pltpu.make_async_remote_copy(
            src_ref=src, dst_ref=dst, send_sem=send, recv_sem=recv, device_id=device, device_id_type=pl.DeviceIdType.MESH
        )

    def half_rows(c):
        return pl.ds(pl.multiple_of(c * half, half), half)

    def slab_rows(c, q):
        return pl.ds(pl.multiple_of(c * half + q * rows, rows), rows)

    def halves(n):
        return slice(0, n // 2), slice(n // 2, n)

    def image_rows(c):
        rows_of_c = split2(w_ref[:, half_rows(c)].T)
        for h in halves(depth):
            x_ref[half_rows(c), h] = product3(rows_of_c, (z1_ref[:, h], z2_ref[:, h]), 1, 0)

    for i in range(LOADS):
        loads[2 * i].wait()
        loads[2 * i + 1].wait()
        parts = split2(z_ref[:, load_part(i)])
        z1_ref[:, load_part(i)], z2_ref[:, load_part(i)] = parts
        start = split2(s_ref[load_part(i), :])
        for upper in halves(z_ref.shape[0]):
            term = product3([p[upper] for p in parts], start, 1, 0)
            w_ref[upper, :] = term if i == 0 else w_ref[upper, :] + term
    image_rows(other)
    pl.semaphore_wait(barrier, len(greet))
    pair = remote(x_ref.at[half_rows(other), :], pair_ref, pair_s, pair_r, at(mq, other, mz))
    pair.start()
    image_rows(mc)
    for h in halves(rank):
        m1_ref[h, :] = contract(s_ref[:, h], s_ref[...], 0, 0)
    pair.wait()
    x_ref[half_rows(mc), :] = x_ref[half_rows(mc), :] + pair_ref[...]

    for i in range(PARTS):
        for j, (dx, dy) in enumerate(plane):
            q = plane_peer(dx, dy)
            remote(
                x_ref.at[slab_rows(mc, q), part(i)], plane_ref.at[i, j, :, width(i)], plane_s.at[i], plane_r.at[i], at(q, mc, mz)
            ).start()

    def plane_all(i, send, recv):
        every = plane_ref.at[i, :, :, width(i)]
        return remote(every, every, send.at[i], recv.at[i], at(mq, other, mz))

    def line_all(i):
        most = line_ref.at[i, pl.ds(0, nz - 1), :, width(i)]
        return remote(most, most, line_s.at[i], line_r.at[i], at(mq, other, mz))

    start_factor = (m1_ref, left1_ref, right1_ref)
    steps = steps_of(start_factor)
    cut1, cut2 = steps * CUT1 // 16, steps * CUT2 // 16
    factor_steps(start_factor, 0, cut1)
    for i in range(PARTS):
        plane_all(i, plane_s, plane_r).wait_recv()
        total = x_ref[slab_rows(mc, mq), part(i)]
        for j in range(len(plane)):
            total = total + plane_ref[i, j, :, width(i)]
        line_ref[i, mz, :, width(i)] = total
        own = line_ref.at[i, mz, :, width(i)]
        for dz in line:
            remote(own, own, line_s.at[i], line_r.at[i], at(mq, mc, (mz + dz) % nz)).start()
    factor_steps(start_factor, cut1, cut2)
    for i in range(PARTS):
        line_all(i).wait_recv()
        full_ref[slab_rows(mc, mq), part(i)] = functools.reduce(jnp.add, [line_ref[i, z, :, width(i)] for z in range(nz)])
        slab = full_ref.at[slab_rows(mc, mq), part(i)]
        for dx, dy in plane:
            remote(slab, slab, back_s.at[i], back_r.at[i], at(plane_peer(dx, dy), mc, mz)).start()
    factor_steps(start_factor, cut2, steps)
    start_inverse = split2(m1_ref[...])
    energy_all = jnp.sum(z_ref[...] * z_ref[...])

    def forward(i):
        block = full_ref.at[half_rows(mc), part(i)]
        return remote(block, block, fw_s.at[i], fw_r.at[i], at(mq, other, mz))

    for i in range(PARTS + 1):
        if i < PARTS:
            plane_all(i, back_s, back_r).wait_recv()
            forward(i).start()
        if i > 0:
            forward(i - 1).wait_recv()
            image = part_ref.at[:, width(i - 1)]
            image[...] = product3(start_inverse, split2(full_ref[:, part(i - 1)]), 1, 0)
            square = contract(image[...], image[...], 1, 1)
            m2_ref[...] = square if i == 1 else m2_ref[...] + square
            term = product3((z1_ref[:, part(i - 1)], z2_ref[:, part(i - 1)]), split2(image[...]), 1, 1)
            w_ref[...] = term if i == 1 else w_ref[...] + term

    image_factor = (m2_ref, left2_ref, right2_ref)
    factor_steps(image_factor, 0, steps_of(image_factor))
    compressed = product3(split2(w_ref[...]), split2(m2_ref[...]), 1, 1)
    c_ref[...] = compressed
    energy_kept = jnp.sum(compressed * compressed)

    lane = lax.broadcasted_iota(jnp.int32, (1, 128), 1)
    e_ref[...] = jnp.where(lane == 0, energy_kept, jnp.where(lane == 1, energy_all, 0.0))
    ep_ref[mq] = e_ref[...]
    first = []
    for j, (dx, dy) in enumerate(plane):
        first.append(remote(e_ref, ep_ref.at[mq], ep_s.at[j], ep_r.at[j], at(plane_peer(dx, dy), mc, mz)))
        first[-1].start()
    for copy in first:
        copy.wait()
    e_ref[...] = functools.reduce(jnp.add, [ep_ref[q] for q in range(nq)])
    spot = mz * 2 + mc
    eq_ref[spot] = e_ref[...]
    second = []
    for j, (dz, dc) in enumerate([(dz, dc) for dc in range(2) for dz in [*line, 0] if dz or dc]):
        second.append(
            remote(e_ref, eq_ref.at[spot], eq_s.at[j], eq_r.at[j], at(mq, (mc + dc) % 2, (mz + dz) % nz))
        )
        second[-1].start()
    for i in range(PARTS):
        plane_all(i, plane_s, plane_r).wait_send()
        line_all(i).wait_send()
        plane_all(i, back_s, back_r).wait_send()
        forward(i).wait_send()
    for copy in second:
        copy.wait()
    sums = functools.reduce(jnp.add, [eq_ref[i] for i in range(2 * nz)])
    tail_ref[...] = 1.0 - sums[:, 0:1] / sums[:, 1:2]


def local(sizes, factor, start_block):
    nx, ny, nz = sizes
    nq = nx * ny
    depth, rank = start_block.shape
    half = rank // 2
    rows, cols = half // nq, depth // sum(WIDTHS) * max(WIDTHS)
    vmem = pl.BlockSpec(memory_space=pltpu.VMEM)
    hbm = pl.BlockSpec(memory_space=pltpu.HBM)
    dma = pltpu.SemaphoreType.DMA
    compressed, tail = pl.pallas_call(
        functools.partial(kernel, sizes),
        out_shape=(
            jax.ShapeDtypeStruct((factor.shape[0], rank), F32),
            jax.ShapeDtypeStruct((1, 1), F32),
        ),
        in_specs=[hbm, hbm],
        out_specs=(vmem, vmem),
        scratch_shapes=[
            pltpu.VMEM(factor.shape, F32),
            pltpu.VMEM(start_block.shape, F32),
            pltpu.VMEM((factor.shape[0], rank), F32),
            pltpu.VMEM((rank, depth), F32),
            pltpu.VMEM((half, depth), F32),
            pltpu.VMEM((PARTS, nq - 1, rows, cols), F32),
            pltpu.VMEM((PARTS, nz, rows, cols), F32),
            pltpu.VMEM((rank, depth), F32),
            pltpu.VMEM((rank, cols), F32),
            pltpu.VMEM(factor.shape, jnp.bfloat16),
            pltpu.VMEM(factor.shape, jnp.bfloat16),
            pltpu.VMEM((rank, rank), F32),
            pltpu.VMEM((rank, 6 * PANEL1), jnp.bfloat16),
            pltpu.VMEM((6 * PANEL1, rank), jnp.bfloat16),
            pltpu.VMEM((rank, rank), F32),
            pltpu.VMEM((rank, 6 * PANEL2), jnp.bfloat16),
            pltpu.VMEM((6 * PANEL2, rank), jnp.bfloat16),
            pltpu.VMEM((1, 128), F32),
            pltpu.VMEM((nq, 1, 128), F32),
            pltpu.VMEM((2 * nz, 1, 128), F32),
            dma((LOADS,)),
            dma((LOADS,)),
            dma,
            dma,
            *[dma((PARTS,)) for _ in range(8)],
            dma((nq - 1,)),
            dma((nq - 1,)),
            dma((2 * nz - 1,)),
            dma((2 * nz - 1,)),
        ],
        compiler_params=pltpu.CompilerParams(
            collective_id=0, has_side_effects=True, vmem_limit_bytes=VMEM_GRANT
        ),
    )(factor, start_block)
    return compressed, tail[0, 0]


def solution(mesh):
    side = math.isqrt(mesh.shape["rows"] // 2)
    sizes = (side, side, mesh.shape["grp"])
    return jax.shard_map(
        functools.partial(local, sizes),
        mesh=mesh,
        in_specs=(P(AXES, None), P()),
        out_specs=(P(AXES, None), P()),
        check_vma=False,
    )
```
